8 devices in a mesh: tp: 2 (over z, y), dp: 4 (over x, core).
Axes of the slice: x: 2, y: 2, z: 1, core: 2. Of those that a mesh axis runs over, the one named last changes fastest.
Arguments:
- hidden: bfloat16 [4, 1024, 576], P('dp')
- norm_w: bfloat16 [576], replicated
- embed: bfloat16 [49152, 576], P('tp')
- targets: int32 [4, 1024], P('dp')
- loss_mask: int32 [4, 1024], P('dp')
- token_ids: int32 [4, 1024], P('dp')
- grad_embed: bfloat16 [4, 1024, 576], P('dp')
Outputs:
- output 1: float32 [], replicated
- output 2: bfloat16 [4, 1024, 576], P('dp')
- output 3: float32 [576], replicated
- output 4: float32 [49152, 576], P('tp', 'dp')
All inputs are finite; a program needn't handle non-finite values.
Results may differ from the reference program's by a relative error of at most 0.001.
Values sent between devices are 32-bit elements.
A program may use at most 1 GiB of HBM per device.

```python
import jax
import jax.numpy as jnp
from jax import lax

VOCAB_SIZE = 49152
D_MODEL = 576
BATCH_SIZE = 4
SEQ_LEN = 1024
ROW_BLOCK = 128
RMS_EPS = 1e-6


def skewed_ids(rand_key, shape):
    key_a, key_b, key_c = jax.random.split(rand_key, 3)
    first = jax.random.randint(key_a, shape, 0, VOCAB_SIZE)
    second = jax.random.randint(key_b, shape, 0, first + 1)
    return jax.random.randint(key_c, shape, 0, second + 1).astype(jnp.int32)


def setup_inputs(seed: int = 0) -> dict:
    key_list = jax.random.split(jax.random.key(seed), 8)
    tokens = BATCH_SIZE * SEQ_LEN
    hidden = jax.random.normal(key_list[0], (BATCH_SIZE, SEQ_LEN, D_MODEL), jnp.float32)
    norm_w = 1.0 + 0.3 * jax.random.normal(key_list[1], (D_MODEL,), jnp.float32)
    embed = (1.5 / D_MODEL ** 0.5) * jax.random.normal(key_list[2], (VOCAB_SIZE, D_MODEL), jnp.float32)
    targets = skewed_ids(key_list[3], (BATCH_SIZE, SEQ_LEN))
    token_ids = skewed_ids(key_list[4], (BATCH_SIZE, SEQ_LEN))
    lengths = jax.random.randint(key_list[5], (BATCH_SIZE, 1), SEQ_LEN // 4, SEQ_LEN + 1)
    loss_mask = (jnp.arange(SEQ_LEN)[None, :] < lengths).astype(jnp.int32)
    grad_embed = (1.5 / tokens) * jax.random.normal(key_list[6], (BATCH_SIZE, SEQ_LEN, D_MODEL), jnp.float32)
    return {"hidden": hidden.astype(jnp.bfloat16), "norm_w": norm_w.astype(jnp.bfloat16), "embed": embed.astype(jnp.bfloat16), "targets": targets, "loss_mask": loss_mask, "token_ids": token_ids, "grad_embed": grad_embed.astype(jnp.bfloat16)}


def reference(hidden, norm_w, embed, targets, loss_mask, token_ids, grad_embed):
    tokens = BATCH_SIZE * SEQ_LEN
    blocks = tokens // ROW_BLOCK
    hidden32 = hidden.reshape(tokens, D_MODEL).astype(jnp.float32)
    norm_gain = norm_w.astype(jnp.float32)

    def rms_norm(rows, weight):
        inv_rms = lax.rsqrt(jnp.mean(rows * rows, axis=-1, keepdims=True) + RMS_EPS)
        return rows * inv_rms * weight

    normed, norm_vjp = jax.vjp(rms_norm, hidden32, norm_gain)
    z_rows = normed.astype(jnp.bfloat16)
    mask_rows = loss_mask.reshape(tokens).astype(jnp.float32)
    token_count = jnp.sum(mask_rows)
    vocab_index = jnp.arange(VOCAB_SIZE)

    def block_step(grad_accum, block_in):
        z_block, target_block, mask_block = block_in
        logits = jnp.dot(z_block, embed.T, preferred_element_type=jnp.float32)
        row_max = jnp.max(logits, axis=-1, keepdims=True)
        log_norm = row_max + jnp.log(jnp.sum(jnp.exp(logits - row_max), axis=-1, keepdims=True))
        is_target = vocab_index[None, :] == target_block[:, None]
        target_logit = jnp.sum(jnp.where(is_target, logits, 0.0), axis=-1, keepdims=True)
        soft_probs = jnp.exp(logits - log_norm)
        dlogits = ((soft_probs - is_target.astype(jnp.float32)) * (mask_block[:, None] / token_count)).astype(jnp.bfloat16)
        grad_z = jnp.dot(dlogits, embed, preferred_element_type=jnp.float32)
        grad_accum = grad_accum + jnp.dot(dlogits.T, z_block, preferred_element_type=jnp.float32)
        loss_part = jnp.sum(mask_block * (log_norm[:, 0] - target_logit[:, 0]))
        return grad_accum, (grad_z, loss_part)

    block_inputs = (z_rows.reshape(blocks, ROW_BLOCK, D_MODEL), targets.reshape(blocks, ROW_BLOCK), mask_rows.reshape(blocks, ROW_BLOCK))
    head_grad, (grad_z_blocks, loss_parts) = lax.scan(block_step, jnp.zeros((VOCAB_SIZE, D_MODEL), jnp.float32), block_inputs)
    grad_z = grad_z_blocks.reshape(tokens, D_MODEL)
    grad_hidden32, grad_gain = norm_vjp(grad_z)
    lookup_grad = jax.ops.segment_sum(grad_embed.reshape(tokens, D_MODEL).astype(jnp.float32), token_ids.reshape(tokens), num_segments=VOCAB_SIZE)
    loss_val = jnp.sum(loss_parts) / token_count
    grad_hidden = grad_hidden32.astype(jnp.bfloat16).reshape(BATCH_SIZE, SEQ_LEN, D_MODEL)
    return (loss_val, grad_hidden, grad_gain, head_grad + lookup_grad)
```

```python
import functools

import jax
import jax.numpy as jnp
from jax import lax
from jax.experimental import pallas as pl
from jax.experimental.pallas import tpu as pltpu
from jax.sharding import PartitionSpec as P


RMS_EPS = 1e-6
LOG2E = 1.4426950408889634
LN2 = 0.6931471805599453
TB = 256
VB = 4096
SC = 512
LB = 1024
CH = 128
LANE = 128
ALL = Ellipsis
MIB = 2**20
SMALL = 2**28
F32 = jnp.float32
BF16 = jnp.bfloat16


def over_lanes(x):
    return jnp.sum(x, axis=1, keepdims=True)


def over_rows(x):
    return jnp.sum(x, axis=0, keepdims=True)


def mean_rows(x):
    return jnp.mean(x, axis=0, keepdims=True)


def cost(flops):
    return pl.CostEstimate(flops=int(flops), bytes_accessed=MIB, transcendentals=0)


def params(vmem_mib, n=2):
    return pltpu.CompilerParams(dimension_semantics=("arbitrary",) * n, vmem_limit_bytes=vmem_mib * MIB)


def stats_stage(l_ref, m_ref, s_ref, row, c):
    for r in range(TB // 8):
        rows = pl.ds(row + 8 * r, 8)
        old = m_ref[rows, :]
        total = s_ref[rows, :]
        parts = [l_ref[0, 0, 8 * r:8 * r + 8, c * SC + LANE * j:c * SC + LANE * j + LANE] for j in range(SC // LANE)]
        new = functools.reduce(jnp.maximum, parts, old)
        total = total * jnp.exp2(old - new)
        for part in parts:
            total = total + jnp.exp2(part - new)
        m_ref[rows, :] = new
        s_ref[rows, :] = total


def logits_kernel(sc, z_ref, e_ref, l_ref, m_ref, s_ref):
    v, t = pl.program_id(0), pl.program_id(1)
    row = pl.multiple_of(sc[0, t] * TB, TB)
    skip = sc[2, 3]

    @pl.when((v == 0) & (t >= skip))
    def _():
        m_ref[pl.ds(row, TB), :] = jnp.full((TB, LANE), -3e38, F32)
        s_ref[pl.ds(row, TB), :] = jnp.zeros((TB, LANE), F32)

    @pl.when(t >= skip)
    def _():
        n = VB // SC
        for c in range(n + 1):
            if c < n:
                q = slice(c * SC, (c + 1) * SC)
                l_ref[0, 0, :, q] = jnp.dot(z_ref[ALL], e_ref[:, q], preferred_element_type=F32) * LOG2E
            if c > 0:
                stats_stage(l_ref, m_ref, s_ref, row, c - 1)


def dlogits_stage(get, dl_ref, k_ref, scale, t_ref, tl_ref, row, base, c):
    for r in range(TB // 16):
        rows = pl.ds(row + 16 * r, 16)
        shift = k_ref[rows, :]
        target = t_ref[rows, :] - base
        if tl_ref is not None:
            found = tl_ref[rows, :]
        for j in range(SC // LANE):
            o = c * SC + LANE * j
            x = get(r, o)
            hit = target == o
            p = jnp.exp2(x - shift)
            if tl_ref is not None:
                found = jnp.where(hit, x, found)
            dl_ref[16 * r:16 * r + 16, o:o + LANE] = jnp.where(hit, p - scale, p).astype(BF16)
        if tl_ref is not None:
            tl_ref[rows, :] = found


def own_kernel(sc, l_ref, e_ref, za_ref, zb_ref, k_ref, t_ref, inv_ref, dz_ref, da_ref, db_ref, tl_ref, dl_ref):
    v, t = pl.program_id(0), pl.program_id(1)
    row = pl.multiple_of(sc[0, t] * TB, TB)
    skip = sc[2, 3]

    @pl.when((v == 0) & (t >= skip))
    def _():
        dz_ref[:, pl.ds(row, TB)] = jnp.zeros((dz_ref.shape[0], TB), F32)

    @pl.when((v == 0) & (t == 0))
    def _():
        tl_ref[ALL] = jnp.zeros_like(tl_ref)

    @pl.when(t == skip)
    def _():
        da_ref[ALL] = jnp.zeros_like(da_ref)
        db_ref[ALL] = jnp.zeros_like(db_ref)

    @pl.when(t >= skip)
    def _():
        zc = jnp.concatenate([za_ref[ALL], zb_ref[ALL]], axis=0)
        half = za_ref.shape[0]
        scale = jnp.concatenate([inv_ref[ALL], inv_ref[ALL]], axis=0)
        n = VB // SC
        get = lambda r, o: l_ref[0, 0, 16 * r:16 * r + 16, o:o + LANE]
        for c in range(n + 1):
            if c < n:
                dlogits_stage(get, dl_ref, k_ref, scale, t_ref, tl_ref, row, v * VB, c)
            if c > 0:
                q = slice((c - 1) * SC, c * SC)
                dl = dl_ref[:, q]
                dz_ref[:, pl.ds(row, TB)] += lax.dot_general(
                    e_ref[:, q], dl, (((1,), (1,)), ((), ())), preferred_element_type=F32)
                de = jnp.dot(zc, dl, preferred_element_type=F32)
                da_ref[:, q] += de[:half]
                db_ref[:, q] += de[half:]


def other_kernel(sc, z_ref, e_ref, za_ref, zb_ref, k_ref, t_ref, inv_ref, ia_ref, ib_ref, da_ref, db_ref, l_ref, dl_ref):
    v, t = pl.program_id(0), pl.program_id(1)
    row = pl.multiple_of(sc[1, t] * TB, TB)
    skip = sc[2, 4]

    @pl.when(t == skip)
    def _():
        da_ref[ALL] = ia_ref[ALL]
        db_ref[ALL] = ib_ref[ALL]

    @pl.when(t >= skip)
    def _():
        zc = jnp.concatenate([za_ref[ALL], zb_ref[ALL]], axis=0)
        half = za_ref.shape[0]
        scale = jnp.concatenate([inv_ref[ALL], inv_ref[ALL]], axis=0)
        n = VB // SC
        get = lambda r, o: l_ref[16 * r:16 * r + 16, o:o + LANE] * LOG2E
        for c in range(n + 2):
            if c < n:
                q = slice(c * SC, (c + 1) * SC)
                l_ref[:, q] = jnp.dot(z_ref[ALL], e_ref[:, q], preferred_element_type=F32)
            if 0 < c <= n:
                dlogits_stage(get, dl_ref, k_ref, scale, t_ref, None, row, v * VB, c - 1)
            if c > 1:
                q = slice((c - 2) * SC, (c - 1) * SC)
                de = jnp.dot(zc, dl_ref[:, q], preferred_element_type=F32)
                da_ref[:, q] += de[:half]
                db_ref[:, q] += de[half:]


def arrange_kernel(idx, a_ref, b_ref, zt_ref, z_ref):
    x = jnp.where(pl.program_id(0) == 0, a_ref[ALL], b_ref[ALL])
    zt_ref[ALL] = x.astype(BF16)
    z_ref[ALL] = x.T.astype(BF16)


def xor(i, k):
    return (i + 1 - 2 * lax.rem(i, 2), lax.rem(i + 2, 4), 3 - i)[k - 1]


def columns(row):
    return jnp.broadcast_to(row, (LANE, LANE)).T


def sort_kernel(t_ref, m_ref, i_ref, ge_ref, o1, o2, o3, o4, meta_ref, key_ref, perm_ref, sorted_ref):
    seq = i_ref.shape[1]
    nb = seq // LANE
    lane = lax.broadcasted_iota(jnp.int32, (1, LANE), 1)
    rows = [i_ref[:, LANE * j:LANE * j + LANE] * seq + lane + LANE * j for j in range(nb)]
    for j in range(nb):
        key_ref[LANE * j:LANE * j + LANE, :] = columns(rows[j])
    keys = key_ref[ALL]
    before = jnp.zeros((seq, LANE), F32)
    for j in range(nb):
        before = before + jnp.where(rows[j] < keys, 1.0, 0.0)
    rank = jnp.broadcast_to(over_lanes(before), (seq, LANE)).astype(jnp.int32)
    meta_ref[ALL] = jnp.zeros_like(meta_ref)
    meta_ref[0:1, :] = t_ref[ALL]
    meta_ref[1:2, :] = m_ref[ALL]
    for j in range(nb):
        hit = rank == lane + LANE * j
        perm_ref[:, LANE * j:LANE * j + LANE] = jnp.where(hit, 1.0, 0.0).astype(BF16)
        place = over_rows(jnp.where(hit, keys, 0))
        meta_ref[2:3, LANE * j:LANE * j + LANE] = lax.shift_right_logical(place, seq.bit_length() - 1)
    sorted_ref[ALL] = jnp.dot(ge_ref[ALL], perm_ref[ALL], preferred_element_type=F32)
    dp = lax.axis_index("dp")
    cols = o1.shape[0]
    for k, o in enumerate((o1, o2, o3, o4)):
        who = dp if k == 0 else xor(dp, k)
        o[ALL] = sorted_ref[pl.ds(pl.multiple_of(who * cols, 8), cols), :]


def greet(peers):
    barrier = pltpu.get_barrier_semaphore()
    for peer in peers:
        pl.semaphore_signal(barrier, inc=1, device_id=peer, device_id_type=pl.DeviceIdType.MESH)
    pl.semaphore_wait(barrier, len(peers))


def send(src, dst, sems, k, peer):
    copy = pltpu.make_async_remote_copy(
        src_ref=src, dst_ref=dst, send_sem=sems[0].at[k], recv_sem=sems[1].at[k],
        device_id=peer, device_id_type=pl.DeviceIdType.MESH)
    copy.start()
    return copy


def prep_kernel(h_ref, g_ref, meta_ref, z32_ref, zt_ref, z_ref, all_ref, table_ref, inv_ref, got_ref, box_ref, s_sem, r_sem):
    dp, tp = lax.axis_index("dp"), lax.axis_index("tp")
    core = lax.rem(dp, 2)
    chip = lax.div(dp, 2)
    _, seq = h_ref.shape
    at = lambda i: (tp, i)
    peers = [at(xor(dp, k)) for k in (1, 2, 3)]
    greet(peers)
    sems = (s_sem, r_sem)
    copies = [send(meta_ref, box_ref.at[k], sems, k, peers[k]) for k in range(3)]
    x = h_ref[ALL].astype(F32)
    inv = lax.rsqrt(mean_rows(x * x) + RMS_EPS)
    gain = jnp.concatenate([g_ref[ALL]] * (seq // LANE), axis=1)
    z = (x * inv * gain).astype(BF16)
    z32_ref[ALL] = z.astype(F32)
    z_ref[pl.ds(pl.multiple_of(core * seq, seq), seq), :] = z.T
    copies.append(send(z32_ref, got_ref, sems, 3, peers[0]))
    zt_ref[:, pl.ds(pl.multiple_of(core * seq, seq), seq)] = z
    for copy in copies[:3]:
        copy.wait()
    all_ref[dp] = meta_ref[ALL]
    for k in range(3):
        all_ref[xor(dp, k + 1)] = box_ref[k]

    tiles = []
    total = jnp.zeros((1, 1), F32)
    for q in range(4):
        length = over_lanes(all_ref[q, 1:2, :].astype(F32))
        total = total + length
        tiles.append(jnp.floor((length + (TB - 1)) * (1.0 / TB)).astype(jnp.int32))
    inv_ref[ALL] = jnp.broadcast_to(1.0 / total, inv_ref.shape)
    nt = 2 * seq // TB
    lane = lax.broadcasted_iota(jnp.int32, (1, LANE), 1)
    swap = chip == 1
    pairs = [(tiles[0], tiles[1]), (tiles[2], tiles[3])]
    out = []
    skips = []
    for c in range(2):
        na = jnp.where(swap, pairs[1 - c][0], pairs[c][0])
        nb = jnp.where(swap, pairs[1 - c][1], pairs[c][1])
        skip = nt - na - nb
        p = jnp.maximum(lane - skip, 0)
        lst = jnp.where(p < na, p, nt // 2 + p - na)
        out.append(jnp.minimum(lst, nt - 1))
        skips.append(skip)
    row = jnp.where(lane == 0, core, jnp.where(lane == 1, dp, jnp.where(lane == 2, xor(dp, 1), jnp.where(lane == 3, skips[0], skips[1]))))
    table_ref[ALL] = jnp.zeros_like(table_ref)
    table_ref[0:1, :] = out[0]
    table_ref[1:2, :] = out[1]
    table_ref[2:3, :] = row

    copies[3].wait()
    other = xor(dp, 1) - 2 * chip
    got = got_ref[ALL].astype(BF16)
    z_ref[pl.ds(pl.multiple_of(other * seq, seq), seq), :] = got.T
    zt_ref[:, pl.ds(pl.multiple_of(other * seq, seq), seq)] = got


def stats_kernel(vocab_local, m_ref, s_ref, all_ref, ko_ref, to_ref, kf_ref, tf_ref, lse_ref, look_ref, mine_ref, box_ref, s_sem, r_sem):
    dp, tp = lax.axis_index("dp"), lax.axis_index("tp")
    core = lax.rem(dp, 2)
    chip = lax.div(dp, 2)
    tokens = m_ref.shape[0]
    seq = all_ref.shape[2]
    nb = tokens // LANE
    dps = [dp, xor(dp, 1), xor(dp, 2), xor(dp, 3)]
    peers = [(t, i) for t in (tp, 1 - tp) for i in dps][1:]
    greet(peers)
    for j in range(nb):
        m = m_ref[LANE * j:LANE * j + LANE, :].T
        s = s_ref[LANE * j:LANE * j + LANE, :].T
        top = jnp.max(m, axis=0, keepdims=True)
        mine_ref[j:j + 1, :] = top
        mine_ref[nb + j:nb + j + 1, :] = over_rows(s * jnp.exp2(m - top))
    box_ref[0] = mine_ref[ALL]
    copies = [send(mine_ref, box_ref.at[k + 1], (s_sem, r_sem), k, peers[k]) for k in range(7)]

    lane = lax.broadcasted_iota(jnp.int32, (1, LANE), 1)
    edge = lane * LB + tp * vocab_local
    look_ref[ALL] = jnp.zeros_like(look_ref)
    steps = jnp.zeros((1, LANE), F32)
    for q in range(4):
        lo = jnp.zeros((1, LANE), F32)
        hi = jnp.zeros((1, LANE), F32)
        for j in range(seq // LANE):
            ids = columns(all_ref[dps[q], 2:3, LANE * j:LANE * j + LANE])
            lo = lo + over_rows(jnp.where(ids < edge, 1.0, 0.0))
            hi = hi + over_rows(jnp.where(ids < edge + LB, 1.0, 0.0))
        a = jnp.floor(lo * (1.0 / CH))
        b = jnp.floor((hi + (CH - 1)) * (1.0 / CH))
        look_ref[q:q + 1, :] = a.astype(jnp.int32)
        steps = jnp.maximum(steps, jnp.where(hi > lo, b - a, 0.0))
    look_ref[4:5, :] = steps.astype(jnp.int32)

    total = jnp.zeros((1, 1), F32)
    for q in range(4):
        total = total + over_lanes(all_ref[q, 1:2, :].astype(F32))
    shift = jnp.log(total) * LOG2E
    for copy in copies:
        copy.wait()

    def merged(slots):
        ms = [box_ref[k, 0:nb, :] for k in slots]
        ss = [box_ref[k, nb:2 * nb, :] for k in slots]
        top = functools.reduce(jnp.maximum, ms)
        w = [s * jnp.exp2(m - top) for s, m in zip(ss, ms)]
        return top + jnp.log((w[0] + w[1]) + (w[2] + w[3])) * LOG2E

    sets = [(merged((0, 1, 4, 5)), chip, ko_ref, to_ref), (merged((2, 3, 6, 7)), 1 - chip, kf_ref, tf_ref)]
    base = tp * vocab_local + core * (vocab_local // 2)
    sums = []
    for lse, c, k_out, t_out in sets:
        acc = jnp.zeros((1, LANE), F32)
        for j in range(nb):
            q, o = c * 2 + j // (nb // 2), LANE * (j % (nb // 2))
            on = all_ref[q, 1:2, o:o + LANE] > 0
            row = lse[j:j + 1, :]
            acc = acc + jnp.where(on, row, 0.0)
            k_out[LANE * j:LANE * j + LANE, :] = columns(jnp.where(on, row + shift, jnp.inf))
            t_out[LANE * j:LANE * j + LANE, :] = columns(jnp.where(on, all_ref[q, 0:1, o:o + LANE] - base, -MIB)) - lane
        sums.append(acc)
    lse_ref[ALL] = jnp.broadcast_to(sums[0] + sums[1], lse_ref.shape)


def final_kernel(a_ref, b_ref, h_ref, g_ref, on_ref, tl_ref, lse_ref, inv_ref, dh_ref, dg_ref, loss_ref, mine_ref, box_ref, s_sem, r_sem):
    dp, tp = lax.axis_index("dp"), lax.axis_index("tp")
    dps = [dp, xor(dp, 1), xor(dp, 2), xor(dp, 3)]
    peers = [(t, i) for t in (tp, 1 - tp) for i in dps][1:]
    greet(peers)
    d, seq = h_ref.shape
    x = h_ref[ALL].astype(F32)
    inv = lax.rsqrt(mean_rows(x * x) + RMS_EPS)
    u = x * inv
    dz = jnp.where(on_ref[ALL] > 0, a_ref[ALL] + b_ref[ALL], 0.0)
    prod = dz * u
    part = sum(prod[:, LANE * j:LANE * j + LANE] for j in range(seq // LANE))
    mine_ref[ALL] = jnp.zeros_like(mine_ref)
    mine_ref[0:1, 0:d] = over_rows(part.T)
    mine_ref[1:2, 0:LANE] = over_rows(tl_ref[ALL])
    gain = jnp.concatenate([g_ref[ALL]] * (seq // LANE), axis=1)
    w = dz * gain
    dh_ref[ALL] = (inv * (w - u * mean_rows(w * u))).astype(BF16)
    box_ref[0] = mine_ref[ALL]
    copies = [send(mine_ref, box_ref.at[k + 1], (s_sem, r_sem), k, peers[k]) for k in range(7)]
    for copy in copies:
        copy.wait()
    same = [jnp.zeros((1, d), F32)] * 4
    found = jnp.zeros((1, LANE), F32)
    for q in range(4):
        row = jnp.zeros((1, d), F32)
        hit = jnp.zeros((1, LANE), F32)
        low = jnp.zeros((1, LANE), F32)
        for k in range(4):
            row = jnp.where(dps[k] == q, box_ref[k, 0:1, 0:d], row)
            hit = jnp.where(dps[k] == q, box_ref[k, 1:2, 0:LANE], hit)
            low = jnp.where(dps[k] == q, box_ref[k + 4, 1:2, 0:LANE], low)
        same[q] = row
        found = found + (hit + low)
    dg_ref[ALL] = same[0] + same[1] + same[2] + same[3]
    loss = over_lanes(lse_ref[0:1, :] - found) * LN2
    loss_ref[ALL] = jnp.broadcast_to(loss, loss_ref.shape) * inv_ref[0:1, :]


def lookup_kernel(top, sc, look, from_ref, g1, g2, g3, g4, all_ref, *rest):
    out_ref, id_ref = rest[-2:]
    b = pl.program_id(0)
    nc = all_ref.shape[2] // CH

    @pl.when(b == 0)
    def _():
        for q in range(4):
            who = sc[2, 1] if q == 0 else xor(sc[2, 1], q)
            for j in range(nc):
                id_ref[q, j] = columns(all_ref[who, 2:3, CH * j:CH * j + CH])

    at = top(sc, b)
    out_ref[ALL] = from_ref[ALL]
    cols = lax.broadcasted_iota(jnp.int32, (CH, LB), 1) + (at * LB + sc[2, 5])

    def step(k, _):
        hots, rows = [], []
        for q, g in enumerate((g1, g2, g3, g4)):
            c = look[q, at] + k
            ok = c < nc
            c = jnp.minimum(c, nc - 1)
            ids = jnp.concatenate([id_ref[q, c]] * (LB // LANE), axis=1)
            hots.append(jnp.where(ids == jnp.where(ok, cols, -1), 1.0, 0.0).astype(BF16))
            rows.append(g[:, pl.ds(pl.multiple_of(c * CH, CH), CH)].astype(BF16))
        out_ref[ALL] += jnp.dot(jnp.concatenate(rows, axis=1), jnp.concatenate(hots, axis=0), preferred_element_type=F32)
        return 0

    lax.fori_loop(0, look[4, at], step, 0)


def solution(mesh):
    n_dp = mesh.shape["dp"]
    swap = {k: [(i, i ^ k) for i in range(n_dp)] for k in (1, 2, 3)}
    whole = pl.BlockSpec(memory_space=pltpu.VMEM)
    shape = jax.ShapeDtypeStruct
    dma = pltpu.SemaphoreType.DMA

    def local_step(hidden, norm_w, embed, targets, loss_mask, token_ids, grad_embed):
        _, seq, d = hidden.shape
        vocab_local = embed.shape[0]
        half = vocab_local // 2
        nv = half // VB
        cols = d // n_dp
        nt = 2 * seq // TB
        et = embed.T
        ht = hidden[0].T
        gain = jnp.broadcast_to(norm_w.astype(F32)[:, None], (d, LANE))
        talk = lambda i, mib: pltpu.CompilerParams(collective_id=i, has_side_effects=True, vmem_limit_bytes=mib * MIB)

        *give, meta = pl.pallas_call(
            sort_kernel, in_specs=[whole] * 4, out_specs=[whole] * 5,
            out_shape=[shape((cols, seq), F32)] * 4 + [shape((8, seq), jnp.int32)],
            scratch_shapes=[pltpu.VMEM((seq, LANE), jnp.int32), pltpu.VMEM((seq, seq), BF16), pltpu.VMEM((d, seq), F32)],
            compiler_params=pltpu.CompilerParams(vmem_limit_bytes=40 * MIB), name="sort",
            cost_estimate=cost(2 * d * seq * seq),
        )(targets, loss_mask, token_ids, grad_embed[0].T)

        zt32, zt_chip, z_chip, metas, table, inv_n = pl.pallas_call(
            prep_kernel, in_specs=[whole] * 3, out_specs=[whole] * 6,
            out_shape=[shape((d, seq), F32), shape((d, 2 * seq), BF16), shape((2 * seq, d), BF16),
                       shape((n_dp, 8, seq), jnp.int32), shape((8, LANE), jnp.int32), shape((8, LANE), F32)],
            scratch_shapes=[pltpu.VMEM((d, seq), F32), pltpu.VMEM((3, 8, seq), jnp.int32), dma((4,)), dma((4,))],
            compiler_params=talk(0, 48), name="prep",
            cost_estimate=cost(SMALL),
        )(ht, gain, meta)
        tp_base = lax.axis_index("tp") * vocab_local
        spot = (lax.broadcasted_iota(jnp.int32, (8, LANE), 0) == 2) & (lax.broadcasted_iota(jnp.int32, (8, LANE), 1) == 5)
        table = jnp.where(spot, tp_base, table)

        far = lax.ppermute(zt32, "dp", swap[2])
        far_near = lax.ppermute(far, "dp", swap[1])

        def arrange(a, b):
            w = 512
            n = seq // w
            place = lambda j, i, x: lax.bitwise_xor(j, x[2, 0]) * n + i
            return pl.pallas_call(
                arrange_kernel,
                grid_spec=pltpu.PrefetchScalarGridSpec(
                    num_scalar_prefetch=1, grid=(2, n),
                    in_specs=[
                        pl.BlockSpec((d, w), lambda j, i, x: (0, jnp.where(j == 0, i, n - 1))),
                        pl.BlockSpec((d, w), lambda j, i, x: (0, jnp.where(j == 1, i, 0)))],
                    out_specs=[
                        pl.BlockSpec((d, w), lambda j, i, x: (0, place(j, i, x))),
                        pl.BlockSpec((w, d), lambda j, i, x: (place(j, i, x), 0))]),
                out_shape=[shape((d, 2 * seq), BF16), shape((2 * seq, d), BF16)],
                compiler_params=params(40), name="arrange",
                cost_estimate=cost(SMALL),
            )(table, a, b)

        def specs(r):
            full = lambda v, t, x: (0, 0)
            return dict(
                e=pl.BlockSpec((d, VB), lambda v, t, x: (0, x[2, 0] * nv + v)),
                z=pl.BlockSpec((TB, d), lambda v, t, x: (x[r, t], 0)),
                l=pl.BlockSpec((1, 1, TB, VB), lambda v, t, x: (x[r, t], v, 0, 0)),
                vec=pl.BlockSpec((2 * seq, LANE), full),
                inv=pl.BlockSpec((8, LANE), full),
                dz=pl.BlockSpec((d, 2 * seq), full),
                za=pl.BlockSpec((cols, TB), lambda v, t, x: (x[2, 1], x[r, t])),
                zb=pl.BlockSpec((cols, TB), lambda v, t, x: (x[2, 2], x[r, t])),
                de=pl.BlockSpec((cols, VB), lambda v, t, x: (0, v)))

        pick = lambda sp, *names: [sp[k] for k in names]
        own, other = specs(0), specs(1)
        vec = shape((2 * seq, LANE), F32)
        ivec = shape((2 * seq, LANE), jnp.int32)
        de_shape = shape((cols, half), F32)
        flops = 2 * 2 * seq * half * d

        l_own, m_own, s_own = pl.pallas_call(
            logits_kernel,
            grid_spec=pltpu.PrefetchScalarGridSpec(
                num_scalar_prefetch=1, grid=(nv, nt), in_specs=pick(own, "z", "e"), out_specs=pick(own, "l", "vec", "vec")),
            out_shape=[shape((nt, nv, TB, VB), F32), vec, vec],
            compiler_params=params(56), name="logits",
            cost_estimate=cost(flops),
        )(table, z_chip, et)

        k_own, t_own, k_far, t_far, lse_sum, look = pl.pallas_call(
            functools.partial(stats_kernel, vocab_local),
            in_specs=[whole] * 3, out_specs=[whole] * 6,
            out_shape=[vec, ivec, vec, ivec, shape((8, LANE), F32), shape((8, LANE), jnp.int32)],
            scratch_shapes=[pltpu.VMEM((4 * seq // LANE, LANE), F32), pltpu.VMEM((8, 4 * seq // LANE, LANE), F32), dma((7,)), dma((7,))],
            compiler_params=talk(1, 32), name="stats",
            cost_estimate=cost(SMALL),
        )(m_own, s_own, metas)

        lists = [give[0]]
        for k in (1, 2, 3):
            lists.append(lax.ppermute(give[k], "dp", swap[k]))

        dz, da, db, tl = pl.pallas_call(
            own_kernel,
            grid_spec=pltpu.PrefetchScalarGridSpec(
                num_scalar_prefetch=1, grid=(nv, nt),
                in_specs=pick(own, "l", "e", "za", "zb", "vec", "vec", "inv"), out_specs=pick(own, "dz", "de", "de", "vec"),
                scratch_shapes=[pltpu.VMEM((TB, VB), BF16)]),
            out_shape=[shape((d, 2 * seq), F32), de_shape, de_shape, vec],
            compiler_params=params(60), name="own",
            cost_estimate=cost(flops + flops // 2),
        )(table, l_own, et, zt_chip, zt_chip, k_own, t_own, inv_n)

        core = lax.rem(lax.axis_index("dp"), 2)
        dz_own = lax.dynamic_slice_in_dim(dz, core * seq, seq, 1)
        dz_give = lax.dynamic_slice_in_dim(dz, (1 - core) * seq, seq, 1)
        dz_near = lax.ppermute(dz_give, "dp", swap[1])
        dz_half = dz_own + dz_near
        dz_tp = lax.ppermute(dz_half, "tp", [(0, 1), (1, 0)])

        zt_far, z_far = arrange(far, far_near)
        da, db = pl.pallas_call(
            other_kernel,
            grid_spec=pltpu.PrefetchScalarGridSpec(
                num_scalar_prefetch=1, grid=(nv, nt),
                in_specs=pick(other, "z", "e", "za", "zb", "vec", "vec", "inv", "de", "de"), out_specs=pick(other, "de", "de"),
                scratch_shapes=[pltpu.VMEM((TB, VB), F32), pltpu.VMEM((TB, VB), BF16)]),
            out_shape=[de_shape, de_shape],
            compiler_params=params(60), name="other",
            cost_estimate=cost(flops + flops // 2),
        )(table, z_far, et, zt_far, zt_far, k_far, t_far, inv_n, da, db)
        got = lax.ppermute(db, "dp", swap[1])

        nb = half // LB

        def lookup(top, source, *prior):
            zero = lambda b, x, k: (0, 0)
            return pl.pallas_call(
                functools.partial(lookup_kernel, top),
                grid_spec=pltpu.PrefetchScalarGridSpec(
                    num_scalar_prefetch=2, grid=(nb,),
                    in_specs=[pl.BlockSpec((cols, LB), lambda b, x, k: (0, b))] + [pl.BlockSpec((cols, seq), zero)] * 4
                    + [pl.BlockSpec((n_dp, 8, seq), lambda b, x, k: (0, 0, 0))] + [pl.BlockSpec(memory_space=pl.ANY)] * len(prior),
                    out_specs=pl.BlockSpec((cols, LB), lambda b, x, k: (0, top(x, b))),
                    scratch_shapes=[pltpu.VMEM((4, seq // CH, CH, LANE), jnp.int32)]),
                out_shape=shape((cols, vocab_local), F32),
                input_output_aliases={8: 0} if prior else {},
                compiler_params=params(40, 1), name="lookup",
                cost_estimate=cost(flops // 8),
            )(table, look, source, *lists, metas, *prior)

        de_t = lookup(lambda x, b: x[2, 0] * nb + b, da)

        dht, dg, loss = pl.pallas_call(
            final_kernel, in_specs=[whole] * 8, out_specs=[whole] * 3,
            out_shape=[shape((d, seq), BF16), shape((1, d), F32), shape((1, LANE), F32)],
            scratch_shapes=[pltpu.VMEM((8, 640), F32), pltpu.VMEM((8, 8, 640), F32), dma((7,)), dma((7,))],
            compiler_params=talk(2, 48), name="final",
            cost_estimate=cost(SMALL),
        )(dz_half, dz_tp, ht, gain, loss_mask, tl, lse_sum, inv_n)

        de_t = lookup(lambda x, b: (1 - x[2, 0]) * nb + b, got, de_t)
        return loss[0, 0], dht.T[None], dg[0], de_t.T

    return jax.shard_map(
        local_step, mesh=mesh,
        in_specs=(P("dp"), P(), P("tp"), P("dp"), P("dp"), P("dp"), P("dp")),
        out_specs=(P(), P("dp"), P(), P("tp", "dp")), check_vma=False)
```

```python
import functools

import jax
import jax.numpy as jnp
from jax import lax
from jax.experimental import pallas as pl
from jax.experimental.pallas import tpu as pltpu
from jax.sharding import PartitionSpec as P


RMS_EPS = 1e-6
LOG2E = 1.4426950408889634
LN2 = 0.6931471805599453
TB = 256
VB = 4096
SC = 512
LB = 1024
CH = 128
LANE = 128
ALL = Ellipsis
MIB = 2**20
SMALL = 2**28
F32 = jnp.float32
BF16 = jnp.bfloat16


def over_lanes(x):
    return jnp.sum(x, axis=1, keepdims=True)


def over_rows(x):
    return jnp.sum(x, axis=0, keepdims=True)


def mean_rows(x):
    return jnp.mean(x, axis=0, keepdims=True)


def cost(flops):
    return pl.CostEstimate(flops=int(flops), bytes_accessed=MIB, transcendentals=0)


def params(vmem_mib, n=2):
    return pltpu.CompilerParams(dimension_semantics=("arbitrary",) * n, vmem_limit_bytes=vmem_mib * MIB)


def stats_stage(l_ref, m_ref, s_ref, row, c):
    for r in range(TB // 8):
        rows = pl.ds(row + 8 * r, 8)
        old = m_ref[rows, :]
        total = s_ref[rows, :]
        parts = [l_ref[0, 0, 8 * r:8 * r + 8, c * SC + LANE * j:c * SC + LANE * j + LANE] for j in range(SC // LANE)]
        new = functools.reduce(jnp.maximum, parts, old)
        total = total * jnp.exp2(old - new)
        for part in parts:
            total = total + jnp.exp2(part - new)
        m_ref[rows, :] = new
        s_ref[rows, :] = total


def logits_kernel(sc, z_ref, e_ref, l_ref, m_ref, s_ref):
    v, t = pl.program_id(0), pl.program_id(1)
    row = pl.multiple_of(sc[0, t] * TB, TB)
    skip = sc[2, 3]

    @pl.when((v == 0) & (t >= skip))
    def _():
        m_ref[pl.ds(row, TB), :] = jnp.full((TB, LANE), -3e38, F32)
        s_ref[pl.ds(row, TB), :] = jnp.zeros((TB, LANE), F32)

    @pl.when(t >= skip)
    def _():
        n = VB // SC
        for c in range(n + 1):
            if c < n:
                q = slice(c * SC, (c + 1) * SC)
                l_ref[0, 0, :, q] = jnp.dot(z_ref[ALL], e_ref[:, q], preferred_element_type=F32) * LOG2E
            if c > 0:
                stats_stage(l_ref, m_ref, s_ref, row, c - 1)


def dlogits_stage(get, dl_ref, k_ref, scale, t_ref, tl_ref, row, base, c):
    for r in range(TB // 16):
        rows = pl.ds(row + 16 * r, 16)
        shift = k_ref[rows, :]
        target = t_ref[rows, :] - base
        if tl_ref is not None:
            found = tl_ref[rows, :]
        for j in range(SC // LANE):
            o = c * SC + LANE * j
            x = get(r, o)
            hit = target == o
            p = jnp.exp2(x - shift)
            if tl_ref is not None:
                found = jnp.where(hit, x, found)
            dl_ref[16 * r:16 * r + 16, o:o + LANE] = jnp.where(hit, p - scale, p).astype(BF16)
        if tl_ref is not None:
            tl_ref[rows, :] = found


def own_kernel(sc, l_ref, e_ref, za_ref, zb_ref, k_ref, t_ref, inv_ref, dz_ref, gv_ref, da_ref, db_ref, tl_ref, dl_ref, kw_ref, tw_ref, acc_ref, sem):
    v, t = pl.program_id(0), pl.program_id(1)
    row = pl.multiple_of(sc[0, t] * TB, TB)
    skip = sc[2, 3]

    expand(t, v, skip, sc[0, t], k_ref, t_ref, kw_ref, tw_ref)
    seq = acc_ref.shape[2]
    slot = lax.bitwise_xor(lax.div(row, seq), sc[2, 0])
    place = pl.ds(pl.multiple_of(lax.rem(row, seq), TB), TB)

    @pl.when((v == 0) & (t >= skip))
    def _():
        acc_ref[slot, :, place] = jnp.zeros((acc_ref.shape[1], TB), F32)

    @pl.when((v == 0) & (t == 0))
    def _():
        tl_ref[ALL] = jnp.zeros_like(tl_ref)

    @pl.when(t == skip)
    def _():
        da_ref[ALL] = jnp.zeros_like(da_ref)
        db_ref[ALL] = jnp.zeros_like(db_ref)

    @pl.when(t >= skip)
    def _():
        zc = jnp.concatenate([za_ref[ALL], zb_ref[ALL]], axis=0)
        half = za_ref.shape[0]
        scale = jnp.concatenate([inv_ref[ALL], inv_ref[ALL]], axis=0)
        n = VB // SC
        get = lambda r, o: l_ref[0, 0, 16 * r:16 * r + 16, o:o + LANE]
        for c in range(n + 1):
            if c < n:
                dlogits_stage(get, dl_ref, kw_ref, scale, tw_ref, tl_ref, row, v * VB, c)
            if c > 0:
                q = slice((c - 1) * SC, c * SC)
                dl = dl_ref[:, q]
                acc_ref[slot, :, place] += lax.dot_general(
                    e_ref[:, q], dl, (((1,), (1,)), ((), ())), preferred_element_type=F32)
                de = jnp.dot(zc, dl, preferred_element_type=F32)
                da_ref[:, q] += de[:half]
                db_ref[:, q] += de[half:]

    @pl.when((v == pl.num_programs(0) - 1) & (t == pl.num_programs(1) - 1))
    def _():
        copies = [pltpu.make_async_copy(acc_ref.at[k], out, sem.at[k]) for k, out in enumerate((dz_ref, gv_ref))]
        for copy in copies:
            copy.start()
        for copy in copies:
            copy.wait()


def other_kernel(sc, z_ref, e_ref, za_ref, zb_ref, k_ref, t_ref, inv_ref, ia_ref, ib_ref, da_ref, db_ref, l_ref, dl_ref, kw_ref, tw_ref):
    v, t = pl.program_id(0), pl.program_id(1)
    row = pl.multiple_of(sc[1, t] * TB, TB)
    skip = sc[2, 4]
    expand(t, v, skip, sc[1, t], k_ref, t_ref, kw_ref, tw_ref)

    @pl.when(t == skip)
    def _():
        da_ref[ALL] = ia_ref[ALL]
        db_ref[ALL] = ib_ref[ALL]

    @pl.when(t >= skip)
    def _():
        zc = jnp.concatenate([za_ref[ALL], zb_ref[ALL]], axis=0)
        half = za_ref.shape[0]
        scale = jnp.concatenate([inv_ref[ALL], inv_ref[ALL]], axis=0)
        n = VB // SC
        get = lambda r, o: l_ref[16 * r:16 * r + 16, o:o + LANE] * LOG2E
        for c in range(n + 2):
            if c < n:
                q = slice(c * SC, (c + 1) * SC)
                l_ref[:, q] = jnp.dot(z_ref[ALL], e_ref[:, q], preferred_element_type=F32)
            if 0 < c <= n:
                dlogits_stage(get, dl_ref, kw_ref, scale, tw_ref, None, row, v * VB, c - 1)
            if c > 1:
                q = slice((c - 2) * SC, (c - 1) * SC)
                de = jnp.dot(zc, dl_ref[:, q], preferred_element_type=F32)
                da_ref[:, q] += de[:half]
                db_ref[:, q] += de[half:]


def arrange_kernel(idx, a_ref, b_ref, zt_ref, z_ref):
    x = jnp.where(pl.program_id(0) == 0, a_ref[ALL], b_ref[ALL])
    zt_ref[ALL] = x.astype(BF16)
    z_ref[ALL] = x.T.astype(BF16)


def xor(i, k):
    return (i + 1 - 2 * lax.rem(i, 2), lax.rem(i + 2, 4), 3 - i)[k - 1]


def expand(t, v, skip, tile, k_ref, t_ref, kw_ref, tw_ref):
    @pl.when((v == 0) & (t >= skip))
    def _():
        lane = lax.broadcasted_iota(jnp.int32, (1, LANE), 1)
        for h in range(TB // LANE):
            r = tile * (TB // LANE) + h
            at = pl.ds(pl.multiple_of(r * LANE, LANE), LANE)
            kw_ref[at, :] = columns(k_ref[pl.ds(r, 1), :])
            tw_ref[at, :] = columns(t_ref[pl.ds(r, 1), :]) - lane


def columns(row):
    return jnp.broadcast_to(row, (LANE, LANE)).T


def sort_kernel(t_ref, m_ref, i_ref, ge_ref, o1, o2, o3, o4, meta_ref, key_ref, perm_ref, sorted_ref):
    seq = i_ref.shape[1]
    nb = seq // LANE
    lane = lax.broadcasted_iota(jnp.int32, (1, LANE), 1)
    rows = [i_ref[:, LANE * j:LANE * j + LANE] * seq + lane + LANE * j for j in range(nb)]
    for j in range(nb):
        key_ref[LANE * j:LANE * j + LANE, :] = columns(rows[j])
    keys = key_ref[ALL]
    before = jnp.zeros((seq, LANE), F32)
    for j in range(nb):
        before = before + jnp.where(rows[j] < keys, 1.0, 0.0)
    rank = jnp.broadcast_to(over_lanes(before), (seq, LANE)).astype(jnp.int32)
    meta_ref[ALL] = jnp.zeros_like(meta_ref)
    meta_ref[0:1, :] = t_ref[ALL]
    meta_ref[1:2, :] = m_ref[ALL]
    for j in range(nb):
        hit = rank == lane + LANE * j
        perm_ref[:, LANE * j:LANE * j + LANE] = jnp.where(hit, 1.0, 0.0).astype(BF16)
        place = over_rows(jnp.where(hit, keys, 0))
        meta_ref[2:3, LANE * j:LANE * j + LANE] = lax.shift_right_logical(place, seq.bit_length() - 1)
    sorted_ref[ALL] = jnp.dot(ge_ref[ALL], perm_ref[ALL], preferred_element_type=F32)
    dp = lax.axis_index("dp")
    cols = o1.shape[0]
    for k, o in enumerate((o1, o2, o3, o4)):
        who = dp if k == 0 else xor(dp, k)
        o[ALL] = sorted_ref[pl.ds(pl.multiple_of(who * cols, 8), cols), :]


def greet(peers):
    barrier = pltpu.get_barrier_semaphore()
    for peer in peers:
        pl.semaphore_signal(barrier, inc=1, device_id=peer, device_id_type=pl.DeviceIdType.MESH)
    pl.semaphore_wait(barrier, len(peers))


def send(src, dst, sems, k, peer):
    copy = pltpu.make_async_remote_copy(
        src_ref=src, dst_ref=dst, send_sem=sems[0].at[k], recv_sem=sems[1].at[k],
        device_id=peer, device_id_type=pl.DeviceIdType.MESH)
    copy.start()
    return copy


def prep_kernel(vocab_local, h_ref, g_ref, meta_ref, z32_ref, zt_ref, z_ref, all_ref, table_ref, inv_ref, got_ref, box_ref, s_sem, r_sem):
    dp, tp = lax.axis_index("dp"), lax.axis_index("tp")
    core = lax.rem(dp, 2)
    chip = lax.div(dp, 2)
    _, seq = h_ref.shape
    at = lambda i: (tp, i)
    peers = [at(xor(dp, k)) for k in (1, 2, 3)]
    greet(peers)
    sems = (s_sem, r_sem)
    copies = [send(meta_ref, box_ref.at[k], sems, k, peers[k]) for k in range(3)]
    x = h_ref[ALL].astype(F32)
    inv = lax.rsqrt(mean_rows(x * x) + RMS_EPS)
    gain = jnp.concatenate([g_ref[ALL]] * (seq // LANE), axis=1)
    z = (x * inv * gain).astype(BF16)
    z32_ref[ALL] = z.astype(F32)
    z_ref[pl.ds(pl.multiple_of(core * seq, seq), seq), :] = z.T
    copies.append(send(z32_ref, got_ref, sems, 3, peers[0]))
    zt_ref[:, pl.ds(pl.multiple_of(core * seq, seq), seq)] = z
    for copy in copies[:3]:
        copy.wait()
    all_ref[dp] = meta_ref[ALL]
    for k in range(3):
        all_ref[xor(dp, k + 1)] = box_ref[k]

    tiles = []
    total = jnp.zeros((1, 1), F32)
    for q in range(4):
        length = over_lanes(all_ref[q, 1:2, :].astype(F32))
        total = total + length
        tiles.append(jnp.floor((length + (TB - 1)) * (1.0 / TB)).astype(jnp.int32))
    inv_ref[ALL] = jnp.broadcast_to(1.0 / total, inv_ref.shape)
    nt = 2 * seq // TB
    lane = lax.broadcasted_iota(jnp.int32, (1, LANE), 1)
    swap = chip == 1
    pairs = [(tiles[0], tiles[1]), (tiles[2], tiles[3])]
    out = []
    skips = []
    for c in range(2):
        na = jnp.where(swap, pairs[1 - c][0], pairs[c][0])
        nb = jnp.where(swap, pairs[1 - c][1], pairs[c][1])
        skip = nt - na - nb
        p = jnp.maximum(lane - skip, 0)
        lst = jnp.where(p < na, p, nt // 2 + p - na)
        out.append(jnp.minimum(lst, nt - 1))
        skips.append(skip)
    row = jnp.where(lane == 0, core, jnp.where(lane == 1, dp, jnp.where(lane == 2, xor(dp, 1), jnp.where(lane == 3, skips[0], jnp.where(lane == 4, skips[1], tp * vocab_local)))))
    table_ref[ALL] = jnp.zeros_like(table_ref)
    table_ref[0:1, :] = out[0]
    table_ref[1:2, :] = out[1]
    table_ref[2:3, :] = row

    copies[3].wait()
    other = xor(dp, 1) - 2 * chip
    got = got_ref[ALL].astype(BF16)
    z_ref[pl.ds(pl.multiple_of(other * seq, seq), seq), :] = got.T
    zt_ref[:, pl.ds(pl.multiple_of(other * seq, seq), seq)] = got


def stats_kernel(vocab_local, m_ref, s_ref, all_ref, k_ref, t_ref, f_ref, lse_ref, look_ref, mine_ref, box_ref, s_sem, r_sem):
    dp, tp = lax.axis_index("dp"), lax.axis_index("tp")
    core = lax.rem(dp, 2)
    chip = lax.div(dp, 2)
    seq = all_ref.shape[2]
    nb = m_ref.shape[0] // LANE
    peers = [(tp, xor(dp, 1)), (1 - tp, dp), (1 - tp, xor(dp, 1))]
    greet(peers)
    for j in range(nb):
        m = m_ref[LANE * j:LANE * j + LANE, :].T
        s = s_ref[LANE * j:LANE * j + LANE, :].T
        top = jnp.max(m, axis=0, keepdims=True)
        mine_ref[j:j + 1, :] = top
        mine_ref[nb + j:nb + j + 1, :] = over_rows(s * jnp.exp2(m - top))
    copies = [send(mine_ref, box_ref.at[k], (s_sem, r_sem), k, peers[k]) for k in range(3)]

    lane = lax.broadcasted_iota(jnp.int32, (1, LANE), 1)
    edge = lane * LB + tp * vocab_local
    look_ref[ALL] = jnp.zeros_like(look_ref)
    steps = jnp.zeros((1, LANE), F32)
    for q in range(4):
        lo = jnp.zeros((1, LANE), F32)
        hi = jnp.zeros((1, LANE), F32)
        who = dp if q == 0 else xor(dp, q)
        for j in range(seq // LANE):
            ids = columns(all_ref[who, 2:3, LANE * j:LANE * j + LANE])
            lo = lo + over_rows(jnp.where(ids < edge, 1.0, 0.0))
            hi = hi + over_rows(jnp.where(ids < edge + LB, 1.0, 0.0))
        a = jnp.floor(lo * (1.0 / CH))
        b = jnp.floor((hi + (CH - 1)) * (1.0 / CH))
        look_ref[q:q + 1, :] = a.astype(jnp.int32)
        steps = jnp.maximum(steps, jnp.where(hi > lo, b - a, 0.0))
    look_ref[4:5, :] = steps.astype(jnp.int32)

    total = sum(over_lanes(all_ref[q, 1:2, :].astype(F32)) for q in range(4))
    shift = jnp.log(total) * LOG2E
    base = tp * vocab_local + core * (vocab_local // 2)
    half = nb // 2
    for c, out in ((chip, t_ref), (1 - chip, f_ref)):
        for j in range(nb):
            q, o = c * 2 + j // half, LANE * (j % half)
            on = all_ref[q, 1:2, o:o + LANE] > 0
            out[j:j + 1, :] = jnp.where(on, all_ref[q, 0:1, o:o + LANE] - base, -MIB)
    for copy in copies:
        copy.wait()
    parts = [mine_ref] + [box_ref.at[k] for k in range(3)]
    ms = [p[0:nb, :] for p in parts]
    top = functools.reduce(jnp.maximum, ms)
    w = [p[nb:2 * nb, :] * jnp.exp2(m - top) for p, m in zip(parts, ms)]
    lse = top + jnp.log((w[0] + w[1]) + (w[2] + w[3])) * LOG2E
    live = t_ref[ALL] > 1 - MIB
    k_ref[ALL] = jnp.where(live, lse + shift, jnp.inf)
    lse_ref[ALL] = jnp.broadcast_to(over_rows(jnp.where(live, lse, 0.0)), lse_ref.shape)


def final_kernel(a_ref, b_ref, h_ref, g_ref, on_ref, tl_ref, lse_ref, inv_ref, dh_ref, dg_ref, loss_ref, mine_ref, box_ref, s_sem, r_sem):
    dp, tp = lax.axis_index("dp"), lax.axis_index("tp")
    dps = [dp, xor(dp, 1), xor(dp, 2), xor(dp, 3)]
    peers = [(t, i) for t in (tp, 1 - tp) for i in dps][1:]
    greet(peers)
    d, seq = h_ref.shape
    x = h_ref[ALL].astype(F32)
    inv = lax.rsqrt(mean_rows(x * x) + RMS_EPS)
    u = x * inv
    dz = jnp.where(on_ref[ALL] > 0, a_ref[ALL] + b_ref[ALL], 0.0)
    prod = dz * u
    part = sum(prod[:, LANE * j:LANE * j + LANE] for j in range(seq // LANE))
    mine_ref[ALL] = jnp.zeros_like(mine_ref)
    mine_ref[0:1, 0:d] = over_rows(part.T)
    mine_ref[1:2, 0:LANE] = over_rows(tl_ref[ALL])
    mine_ref[2:3, 0:LANE] = lse_ref[0:1, :]
    gain = jnp.concatenate([g_ref[ALL]] * (seq // LANE), axis=1)
    w = dz * gain
    dh_ref[ALL] = (inv * (w - u * mean_rows(w * u))).astype(BF16)
    box_ref[0] = mine_ref[ALL]
    copies = [send(mine_ref, box_ref.at[k + 1], (s_sem, r_sem), k, peers[k]) for k in range(7)]
    for copy in copies:
        copy.wait()
    same = [jnp.zeros((1, d), F32)] * 4
    found = jnp.zeros((1, LANE), F32)
    for q in range(4):
        row = jnp.zeros((1, d), F32)
        hit = jnp.zeros((1, LANE), F32)
        low = jnp.zeros((1, LANE), F32)
        for k in range(4):
            row = jnp.where(dps[k] == q, box_ref[k, 0:1, 0:d], row)
            hit = jnp.where(dps[k] == q, box_ref[k, 1:2, 0:LANE], hit)
            low = jnp.where(dps[k] == q, box_ref[k + 4, 1:2, 0:LANE], low)
        same[q] = row
        found = found + (hit + low)
    dg_ref[ALL] = same[0] + same[1] + same[2] + same[3]
    loss = over_lanes(box_ref[0, 2:3, 0:LANE] + box_ref[2, 2:3, 0:LANE] - found) * LN2
    loss_ref[ALL] = jnp.broadcast_to(loss, loss_ref.shape) * inv_ref[0:1, :]


def lookup_kernel(top, sc, look, from_ref, g1, g2, g3, g4, all_ref, *rest):
    out_ref, id_ref = rest[-2:]
    b = pl.program_id(0)
    nc = all_ref.shape[2] // CH

    @pl.when(b == 0)
    def _():
        for q in range(4):
            who = sc[2, 1] if q == 0 else xor(sc[2, 1], q)
            for j in range(nc):
                id_ref[q, j] = columns(all_ref[who, 2:3, CH * j:CH * j + CH])

    at = top(sc, b)
    out_ref[ALL] = from_ref[ALL]
    cols = lax.broadcasted_iota(jnp.int32, (CH, LB), 1) + (at * LB + sc[2, 5])

    def step(k, _):
        hots, rows = [], []
        for q, g in enumerate((g1, g2, g3, g4)):
            c = look[q, at] + k
            ok = c < nc
            c = jnp.minimum(c, nc - 1)
            ids = jnp.concatenate([id_ref[q, c]] * (LB // LANE), axis=1)
            hots.append(jnp.where(ids == jnp.where(ok, cols, -1), 1.0, 0.0).astype(BF16))
            rows.append(g[:, pl.ds(pl.multiple_of(c * CH, CH), CH)].astype(BF16))
        out_ref[ALL] += jnp.dot(jnp.concatenate(rows, axis=1), jnp.concatenate(hots, axis=0), preferred_element_type=F32)
        return 0

    lax.fori_loop(0, look[4, at], step, 0)


def solution(mesh):
    n_dp = mesh.shape["dp"]
    swap = {k: [(i, i ^ k) for i in range(n_dp)] for k in (1, 2, 3)}

    def blocks(*arrays):
        return [pl.BlockSpec(a.shape, lambda i, n=len(a.shape): (0,) * n) for a in arrays]

    shape = jax.ShapeDtypeStruct

    def single(kernel, args, outs, scratch, mib, ident=None):
        talk = {} if ident is None else dict(collective_id=ident, has_side_effects=True)
        return pl.pallas_call(
            kernel, grid=(1,), in_specs=blocks(*args), out_specs=blocks(*outs), out_shape=outs, scratch_shapes=scratch,
            compiler_params=pltpu.CompilerParams(dimension_semantics=("arbitrary",), vmem_limit_bytes=mib * MIB, **talk),
            cost_estimate=cost(SMALL))(*args)

    dma = pltpu.SemaphoreType.DMA

    def local_step(hidden, norm_w, embed, targets, loss_mask, token_ids, grad_embed):
        _, seq, d = hidden.shape
        vocab_local = embed.shape[0]
        half = vocab_local // 2
        nv = half // VB
        cols = d // n_dp
        nt = 2 * seq // TB
        et = embed.T
        ht = hidden[0].T
        gain = jnp.broadcast_to(norm_w.astype(F32)[:, None], (d, LANE))

        *give, meta = single(
            sort_kernel, (targets, loss_mask, token_ids, grad_embed[0].T),
            [shape((cols, seq), F32)] * 4 + [shape((8, seq), jnp.int32)],
            [pltpu.VMEM((seq, LANE), jnp.int32), pltpu.VMEM((seq, seq), BF16), pltpu.VMEM((d, seq), F32)], 48)

        zt32, zt_chip, z_chip, metas, table, inv_n = single(
            functools.partial(prep_kernel, vocab_local), (ht, gain, meta),
            [shape((d, seq), F32), shape((d, 2 * seq), BF16), shape((2 * seq, d), BF16),
             shape((n_dp, 8, seq), jnp.int32), shape((8, LANE), jnp.int32), shape((8, LANE), F32)],
            [pltpu.VMEM((d, seq), F32), pltpu.VMEM((3, 8, seq), jnp.int32), dma((4,)), dma((4,))], 56, 0)

        far = lax.ppermute(zt32, "dp", swap[2])
        far_near = lax.ppermute(far, "dp", swap[1])

        def arrange(a, b):
            w = 512
            n = seq // w
            place = lambda j, i, x: lax.bitwise_xor(j, x[2, 0]) * n + i
            return pl.pallas_call(
                arrange_kernel,
                grid_spec=pltpu.PrefetchScalarGridSpec(
                    num_scalar_prefetch=1, grid=(2, n),
                    in_specs=[
                        pl.BlockSpec((d, w), lambda j, i, x: (0, jnp.where(j == 0, i, n - 1))),
                        pl.BlockSpec((d, w), lambda j, i, x: (0, jnp.where(j == 1, i, 0)))],
                    out_specs=[
                        pl.BlockSpec((d, w), lambda j, i, x: (0, place(j, i, x))),
                        pl.BlockSpec((w, d), lambda j, i, x: (place(j, i, x), 0))]),
                out_shape=[shape((d, 2 * seq), BF16), shape((2 * seq, d), BF16)],
                compiler_params=params(40), name="arrange",
                cost_estimate=cost(SMALL),
            )(table, a, b)

        def specs(r):
            full = lambda v, t, x: (0, 0)
            return dict(
                e=pl.BlockSpec((d, VB), lambda v, t, x: (0, x[2, 0] * nv + v)),
                z=pl.BlockSpec((TB, d), lambda v, t, x: (x[r, t], 0)),
                l=pl.BlockSpec((1, 1, TB, VB), lambda v, t, x: (x[r, t], v, 0, 0)),
                vec=pl.BlockSpec((2 * seq, LANE), full),
                row=pl.BlockSpec((2 * seq // LANE, LANE), full),
                any=pl.BlockSpec(memory_space=pl.ANY),
                inv=pl.BlockSpec((8, LANE), full),
                za=pl.BlockSpec((cols, TB), lambda v, t, x: (x[2, 1], x[r, t])),
                zb=pl.BlockSpec((cols, TB), lambda v, t, x: (x[2, 2], x[r, t])),
                de=pl.BlockSpec((cols, VB), lambda v, t, x: (0, v)))

        pick = lambda sp, *names: [sp[k] for k in names]
        own, other = specs(0), specs(1)
        vec = shape((2 * seq, LANE), F32)
        wide = [pltpu.VMEM((2 * seq, LANE), F32), pltpu.VMEM((2 * seq, LANE), jnp.int32)]
        de_shape = shape((cols, half), F32)
        flops = 2 * 2 * seq * half * d

        l_own, m_own, s_own = pl.pallas_call(
            logits_kernel,
            grid_spec=pltpu.PrefetchScalarGridSpec(
                num_scalar_prefetch=1, grid=(nv, nt), in_specs=pick(own, "z", "e"), out_specs=pick(own, "l", "vec", "vec")),
            out_shape=[shape((nt, nv, TB, VB), F32), vec, vec],
            compiler_params=params(56), name="logits",
            cost_estimate=cost(flops),
        )(table, z_chip, et)

        rows = 2 * seq // LANE
        k_own, t_own, t_far, lse_sum, look = single(
            functools.partial(stats_kernel, vocab_local), (m_own, s_own, metas),
            [shape((rows, LANE), F32), shape((rows, LANE), jnp.int32), shape((rows, LANE), jnp.int32),
             shape((8, LANE), F32), shape((8, LANE), jnp.int32)],
            [pltpu.VMEM((2 * rows, LANE), F32), pltpu.VMEM((3, 2 * rows, LANE), F32), dma((3,)), dma((3,))], 32, 1)
        k_far = lax.ppermute(k_own, "dp", swap[2])

        lists = [give[0]]
        for k in (1, 2, 3):
            lists.append(lax.ppermute(give[k], "dp", swap[k]))

        dz_own, dz_give, da, db, tl = pl.pallas_call(
            own_kernel,
            grid_spec=pltpu.PrefetchScalarGridSpec(
                num_scalar_prefetch=1, grid=(nv, nt),
                in_specs=pick(own, "l", "e", "za", "zb", "row", "row", "inv"), out_specs=pick(own, "any", "any", "de", "de", "vec"),
                scratch_shapes=[pltpu.VMEM((TB, VB), BF16), *wide, pltpu.VMEM((2, d, seq), F32), dma((2,))]),
            out_shape=[shape((d, seq), F32), shape((d, seq), F32), de_shape, de_shape, vec],
            compiler_params=params(60), name="own",
            cost_estimate=cost(flops + flops // 2),
        )(table, l_own, et, zt_chip, zt_chip, k_own, t_own, inv_n)

        dz_near = lax.ppermute(dz_give, "dp", swap[1])
        dz_half = dz_own + dz_near
        dz_tp = lax.ppermute(dz_half, "tp", [(0, 1), (1, 0)])

        zt_far, z_far = arrange(far, far_near)
        da, db = pl.pallas_call(
            other_kernel,
            grid_spec=pltpu.PrefetchScalarGridSpec(
                num_scalar_prefetch=1, grid=(nv, nt),
                in_specs=pick(other, "z", "e", "za", "zb", "row", "row", "inv", "de", "de"), out_specs=pick(other, "de", "de"),
                scratch_shapes=[pltpu.VMEM((TB, VB), F32), pltpu.VMEM((TB, VB), BF16), *wide]),
            out_shape=[de_shape, de_shape],
            compiler_params=params(60), name="other",
            cost_estimate=cost(flops + flops // 2),
        )(table, z_far, et, zt_far, zt_far, k_far, t_far, inv_n, da, db)
        got = lax.ppermute(db, "dp", swap[1])

        nb = half // LB

        def lookup(top, source, *prior):
            zero = lambda b, x, k: (0, 0)
            return pl.pallas_call(
                functools.partial(lookup_kernel, top),
                grid_spec=pltpu.PrefetchScalarGridSpec(
                    num_scalar_prefetch=2, grid=(nb,),
                    in_specs=[pl.BlockSpec((cols, LB), lambda b, x, k: (0, b))] + [pl.BlockSpec((cols, seq), zero)] * 4
                    + [pl.BlockSpec((n_dp, 8, seq), lambda b, x, k: (0, 0, 0))] + [pl.BlockSpec(memory_space=pl.ANY)] * len(prior),
                    out_specs=pl.BlockSpec((cols, LB), lambda b, x, k: (0, top(x, b))),
                    scratch_shapes=[pltpu.VMEM((4, seq // CH, CH, LANE), jnp.int32)]),
                out_shape=shape((cols, vocab_local), F32),
                input_output_aliases={8: 0} if prior else {},
                compiler_params=params(40, 1), name="lookup",
                cost_estimate=cost(flops // 8),
            )(table, look, source, *lists, metas, *prior)

        de_t = lookup(lambda x, b: x[2, 0] * nb + b, da)

        dht, dg, loss = single(
            final_kernel, (dz_half, dz_tp, ht, gain, loss_mask, tl, lse_sum, inv_n),
            [shape((d, seq), BF16), shape((1, d), F32), shape((1, LANE), F32)],
            [pltpu.VMEM((8, 640), F32), pltpu.VMEM((8, 8, 640), F32), dma((7,)), dma((7,))], 56, 2)

        de_t = lookup(lambda x, b: (1 - x[2, 0]) * nb + b, got, de_t)
        return loss[0, 0], dht.T[None], dg[0], de_t.T

    return jax.shard_map(
        local_step, mesh=mesh,
        in_specs=(P("dp"), P(), P("tp"), P("dp"), P("dp"), P("dp"), P("dp")),
        out_specs=(P(), P("dp"), P(), P("tp", "dp")), check_vma=False)
```

```python
import functools

import jax
import jax.numpy as jnp
from jax import lax
from jax.experimental import pallas as pl
from jax.experimental.pallas import tpu as pltpu
from jax.sharding import PartitionSpec as P


RMS_EPS = 1e-6
LOG2E = 1.4426950408889634
LN2 = 0.6931471805599453
TB = 256
VB = 6144
SC = 512
SF = 1024
LW = 2048
LB = 1024
CH = 128
ST = 16
LANE = 128
ALL = Ellipsis
MIB = 2**20
SMALL = 2**28
GRANT = 60 * 1024 * 1024
F32 = jnp.float32
BF16 = jnp.bfloat16


def over_lanes(x):
    return jnp.sum(x, axis=1, keepdims=True)


def over_rows(x):
    return jnp.sum(x, axis=0, keepdims=True)


def mean_rows(x):
    return jnp.mean(x, axis=0, keepdims=True)


def cost(flops):
    return pl.CostEstimate(flops=int(flops), bytes_accessed=MIB, transcendentals=0)


def params(n=2):
    return pltpu.CompilerParams(dimension_semantics=("arbitrary",) * n, vmem_limit_bytes=GRANT)


def stats_stage(l_ref, m_ref, s_ref, row, c):
    for r in range(TB // 8):
        rows = pl.ds(row + 8 * r, 8)
        old = m_ref[rows, :]
        total = s_ref[rows, :]
        parts = [l_ref[0, 0, 8 * r:8 * r + 8, c * SC + LANE * j:c * SC + LANE * j + LANE] for j in range(SC // LANE)]
        new = functools.reduce(jnp.maximum, parts, old)
        total = total * jnp.exp2(old - new)
        for part in parts:
            total = total + jnp.exp2(part - new)
        m_ref[rows, :] = new
        s_ref[rows, :] = total


def logits_kernel(sc, z_ref, e_ref, l_ref, m_ref, s_ref):
    v, t = pl.program_id(0), pl.program_id(1)
    row = pl.multiple_of(sc[0, t] * TB, TB)
    skip = sc[2, 3]

    @pl.when((v == 0) & (t >= skip))
    def _():
        m_ref[pl.ds(row, TB), :] = jnp.full((TB, LANE), -3e38, F32)
        s_ref[pl.ds(row, TB), :] = jnp.zeros((TB, LANE), F32)

    @pl.when(t >= skip)
    def _():
        n = VB // SC
        for c in range(n + 1):
            if c < n:
                q = slice(c * SC, (c + 1) * SC)
                l_ref[0, 0, :, q] = jnp.dot(z_ref[ALL], e_ref[:, q], preferred_element_type=F32) * LOG2E
            if c > 0:
                stats_stage(l_ref, m_ref, s_ref, row, c - 1)


def dlogits_stage(get, dl_ref, k_ref, scale, t_ref, tl_ref, row, base, c, width):
    for r in range(TB // 16):
        rows = pl.ds(row + 16 * r, 16)
        shift = k_ref[rows, :]
        target = t_ref[rows, :] - base
        if tl_ref is not None:
            found = tl_ref[rows, :]
        for j in range(width // LANE):
            o = c * width + LANE * j
            x = get(r, o)
            hit = target == o
            p = jnp.exp2(x - shift)
            if tl_ref is not None:
                found = jnp.where(hit, x, found)
            dl_ref[16 * r:16 * r + 16, o:o + LANE] = jnp.where(hit, p - scale, p).astype(BF16)
        if tl_ref is not None:
            tl_ref[rows, :] = found


def own_kernel(sc, l_ref, e_ref, za_ref, zb_ref, k_ref, t_ref, inv_ref, dz_ref, gv_ref, da_ref, db_ref, tl_ref, dl_ref, kw_ref, tw_ref, acc_ref, sem):
    v, t = pl.program_id(0), pl.program_id(1)
    row = pl.multiple_of(sc[0, t] * TB, TB)
    skip = sc[2, 3]

    expand(t, v, skip, sc[0, t], k_ref, t_ref, kw_ref, tw_ref)
    seq = acc_ref.shape[2]
    slot = lax.bitwise_xor(lax.div(row, seq), sc[2, 0])
    place = pl.ds(pl.multiple_of(lax.rem(row, seq), TB), TB)

    @pl.when((v == 0) & (t >= skip))
    def _():
        acc_ref[slot, :, place] = jnp.zeros((acc_ref.shape[1], TB), F32)

    @pl.when((v == 0) & (t == 0))
    def _():
        tl_ref[ALL] = jnp.zeros_like(tl_ref)

    @pl.when(t == skip)
    def _():
        da_ref[ALL] = jnp.zeros_like(da_ref)
        db_ref[ALL] = jnp.zeros_like(db_ref)

    @pl.when(t >= skip)
    def _():
        zc = jnp.concatenate([za_ref[ALL], zb_ref[ALL]], axis=0)
        half = za_ref.shape[0]
        scale = jnp.concatenate([inv_ref[ALL], inv_ref[ALL]], axis=0)
        n = VB // SC
        get = lambda r, o: l_ref[0, 0, 16 * r:16 * r + 16, o:o + LANE]
        for c in range(n + 1):
            if c < n:
                dlogits_stage(get, dl_ref, kw_ref, scale, tw_ref, tl_ref, row, v * VB, c, SC)
            if c > 0:
                q = slice((c - 1) * SC, c * SC)
                dl = dl_ref[:, q]
                acc_ref[slot, :, place] += lax.dot_general(
                    e_ref[:, q], dl, (((1,), (1,)), ((), ())), preferred_element_type=F32)
                de = jnp.dot(zc, dl, preferred_element_type=F32)
                da_ref[:, q] += de[:half]
                db_ref[:, q] += de[half:]

    @pl.when((v == pl.num_programs(0) - 1) & (t == pl.num_programs(1) - 1))
    def _():
        copies = [pltpu.make_async_copy(acc_ref.at[k], out, sem.at[k]) for k, out in enumerate((dz_ref, gv_ref))]
        for copy in copies:
            copy.start()
        for copy in copies:
            copy.wait()


def other_kernel(sc, z_ref, e_ref, za_ref, zb_ref, k_ref, t_ref, inv_ref, ia_ref, ib_ref, da_ref, db_ref, l_ref, dl_ref, kw_ref, tw_ref):
    v, t = pl.program_id(0), pl.program_id(1)
    row = pl.multiple_of(sc[1, t] * TB, TB)
    skip = sc[2, 4]
    expand(t, v, skip, sc[1, t], k_ref, t_ref, kw_ref, tw_ref)

    @pl.when(t == skip)
    def _():
        da_ref[ALL] = ia_ref[ALL]
        db_ref[ALL] = ib_ref[ALL]

    @pl.when(t >= skip)
    def _():
        zc = jnp.concatenate([za_ref[ALL], zb_ref[ALL]], axis=0)
        half = za_ref.shape[0]
        scale = jnp.concatenate([inv_ref[ALL], inv_ref[ALL]], axis=0)
        n = VB // SF
        get = lambda r, o: l_ref[16 * r:16 * r + 16, o:o + LANE] * LOG2E
        for c in range(n + 2):
            if c < n:
                q = slice(c * SF, (c + 1) * SF)
                l_ref[:, q] = jnp.dot(z_ref[ALL], e_ref[:, q], preferred_element_type=F32)
            if 0 < c <= n:
                dlogits_stage(get, dl_ref, kw_ref, scale, tw_ref, None, row, v * VB, c - 1, SF)
            if c > 1:
                q = slice((c - 2) * SF, (c - 1) * SF)
                de = jnp.dot(zc, dl_ref[:, q], preferred_element_type=F32)
                da_ref[:, q] += de[:half]
                db_ref[:, q] += de[half:]


def swap_kernel(own_ref, give_ref, a_ref, b_ref, zt_ref, z_ref, dz_ref, got_ref, s_sem, r_sem):
    dp, tp = lax.axis_index("dp"), lax.axis_index("tp")
    i, n = pl.program_id(0), pl.num_programs(0)
    peer = (tp, xor(dp, 1))
    copy = link(give_ref, got_ref, (s_sem, r_sem), 0, peer)

    @pl.when(i == 0)
    def _():
        greet([peer])
        copy.start()

    z = jnp.where(i < 4, a_ref[ALL], b_ref[ALL]).astype(BF16)
    zt_ref[ALL] = z
    z_ref[ALL] = z.T

    @pl.when(i == n - 1)
    def _():
        copy.wait()
        dz_ref[ALL] = own_ref[ALL] + got_ref[ALL]


def xor(i, k):
    return (i + 1 - 2 * lax.rem(i, 2), lax.rem(i + 2, 4), 3 - i)[k - 1]


def expand(t, v, skip, tile, k_ref, t_ref, kw_ref, tw_ref):
    @pl.when((v == 0) & (t >= skip))
    def _():
        lane = lax.broadcasted_iota(jnp.int32, (1, LANE), 1)
        for h in range(TB // LANE):
            r = tile * (TB // LANE) + h
            at = pl.ds(pl.multiple_of(r * LANE, LANE), LANE)
            kw_ref[at, :] = columns(k_ref[pl.ds(r, 1), :])
            tw_ref[at, :] = columns(t_ref[pl.ds(r, 1), :]) - lane


def columns(row):
    return jnp.broadcast_to(row, (LANE, LANE)).T


def sort_lists(i_ref, ge_ref, outs, ids_ref, key_ref, perm_ref, sorted_ref):
    seq = i_ref.shape[1]
    nb = seq // LANE
    lane = lax.broadcasted_iota(jnp.int32, (1, LANE), 1)
    rows = [i_ref[:, LANE * j:LANE * j + LANE] * seq + lane + LANE * j for j in range(nb)]
    for j in range(nb):
        key_ref[LANE * j:LANE * j + LANE, :] = columns(rows[j])
    keys = key_ref[ALL]
    before = jnp.zeros((seq, LANE), F32)
    for j in range(nb):
        before = before + jnp.where(rows[j] < keys, 1.0, 0.0)
    rank = jnp.broadcast_to(over_lanes(before), (seq, LANE)).astype(jnp.int32)
    ids_ref[ALL] = jnp.zeros_like(ids_ref)
    for j in range(nb):
        hit = rank == lane + LANE * j
        perm_ref[:, LANE * j:LANE * j + LANE] = jnp.where(hit, 1.0, 0.0).astype(BF16)
        place = over_rows(jnp.where(hit, keys, 0))
        ids_ref[0:1, LANE * j:LANE * j + LANE] = lax.shift_right_logical(place, seq.bit_length() - 1)
    sorted_ref[ALL] = jnp.dot(ge_ref[ALL], perm_ref[ALL], preferred_element_type=F32)
    dp = lax.axis_index("dp")
    cols = outs[0].shape[0]
    for k, o in enumerate(outs):
        who = dp if k == 0 else xor(dp, k)
        o[ALL] = sorted_ref[pl.ds(pl.multiple_of(who * cols, 8), cols), :]


def greet(peers):
    barrier = pltpu.get_barrier_semaphore()
    for peer in peers:
        pl.semaphore_signal(barrier, inc=1, device_id=peer, device_id_type=pl.DeviceIdType.MESH)
    pl.semaphore_wait(barrier, len(peers))


def send(src, dst, sems, k, peer):
    copy = link(src, dst, sems, k, peer)
    copy.start()
    return copy


def link(src, dst, sems, k, peer):
    return pltpu.make_async_remote_copy(
        src_ref=src, dst_ref=dst, send_sem=sems[0].at[k], recv_sem=sems[1].at[k],
        device_id=peer, device_id_type=pl.DeviceIdType.MESH)


def prep_kernel(vocab_local, h_ref, g_ref, t_ref, m_ref, i_ref, ge_ref, z32_ref, zt_ref, z_ref, all_ref, table_ref, inv_ref, o1, o2, o3, o4,
                meta_ref, ids_ref, key_ref, perm_ref, sorted_ref, got_ref, box_ref, id_box_ref, s_sem, r_sem):
    dp, tp = lax.axis_index("dp"), lax.axis_index("tp")
    core = lax.rem(dp, 2)
    chip = lax.div(dp, 2)
    d, seq = h_ref.shape
    at = lambda i: (tp, i)
    peers = [at(xor(dp, k)) for k in (1, 2, 3)]
    meta_ref[ALL] = jnp.zeros_like(meta_ref)
    meta_ref[0:1, :] = t_ref[ALL]
    meta_ref[1:2, :] = m_ref[ALL]
    greet(peers)
    sems = (s_sem, r_sem)
    copies = [send(meta_ref, box_ref.at[k], sems, k, peers[k]) for k in range(3)]
    x = h_ref[ALL].astype(F32)
    inv = lax.rsqrt(mean_rows(x * x) + RMS_EPS)
    gain = jnp.concatenate([jnp.broadcast_to(g_ref[ALL].astype(F32)[None], (LANE, d)).T] * (seq // LANE), axis=1)
    z = (x * inv * gain).astype(BF16)
    z32_ref[ALL] = z.astype(F32)
    z_ref[pl.ds(pl.multiple_of(core * seq, seq), seq), :] = z.T
    copies.append(send(z32_ref, got_ref, sems, 3, peers[0]))
    zt_ref[:, pl.ds(pl.multiple_of(core * seq, seq), seq)] = z
    sort_lists(i_ref, ge_ref, (o1, o2, o3, o4), ids_ref, key_ref, perm_ref, sorted_ref)
    id_copies = [send(ids_ref, id_box_ref.at[k], sems, k + 4, peers[k]) for k in range(3)]
    for copy in copies[:3]:
        copy.wait()
    all_ref[dp] = meta_ref[ALL]
    for k in range(3):
        all_ref[xor(dp, k + 1)] = box_ref[k]

    tiles = []
    total = jnp.zeros((1, 1), F32)
    for q in range(4):
        length = over_lanes(all_ref[q, 1:2, :].astype(F32))
        total = total + length
        tiles.append(jnp.floor((length + (TB - 1)) * (1.0 / TB)).astype(jnp.int32))
    inv_ref[ALL] = jnp.broadcast_to(1.0 / total, inv_ref.shape)
    nt = 2 * seq // TB
    lane = lax.broadcasted_iota(jnp.int32, (1, LANE), 1)
    swap = chip == 1
    pairs = [(tiles[0], tiles[1]), (tiles[2], tiles[3])]
    out = []
    skips = []
    for c in range(2):
        na = jnp.where(swap, pairs[1 - c][0], pairs[c][0])
        nb = jnp.where(swap, pairs[1 - c][1], pairs[c][1])
        skip = nt - na - nb
        p = jnp.maximum(lane - skip, 0)
        lst = jnp.where(p < na, p, nt // 2 + p - na)
        out.append(jnp.minimum(lst, nt - 1))
        skips.append(skip)
    row = jnp.where(lane == 0, core, jnp.where(lane == 1, dp, jnp.where(lane == 2, xor(dp, 1), jnp.where(lane == 3, skips[0], jnp.where(lane == 4, skips[1], tp * vocab_local)))))
    table_ref[ALL] = jnp.zeros_like(table_ref)
    table_ref[0:1, :] = out[0]
    table_ref[1:2, :] = out[1]
    table_ref[2:3, :] = row

    copies[3].wait()
    other = xor(dp, 1) - 2 * chip
    got = got_ref[ALL].astype(BF16)
    z_ref[pl.ds(pl.multiple_of(other * seq, seq), seq), :] = got.T
    zt_ref[:, pl.ds(pl.multiple_of(other * seq, seq), seq)] = got
    for copy in id_copies:
        copy.wait()
    all_ref[dp, 2:3, :] = ids_ref[0:1, :]
    for k in range(3):
        all_ref[xor(dp, k + 1), 2:3, :] = id_box_ref[k, 0:1, :]


def stats_kernel(vocab_local, m_ref, s_ref, all_ref, k_ref, t_ref, f_ref, lse_ref, look_ref, mine_ref, box_ref, s_sem, r_sem):
    dp, tp = lax.axis_index("dp"), lax.axis_index("tp")
    core = lax.rem(dp, 2)
    chip = lax.div(dp, 2)
    seq = all_ref.shape[2]
    nb = m_ref.shape[0] // LANE
    peers = [(tp, xor(dp, 1)), (1 - tp, dp), (1 - tp, xor(dp, 1))]
    greet(peers)
    for j in range(nb):
        m = m_ref[LANE * j:LANE * j + LANE, :].T
        s = s_ref[LANE * j:LANE * j + LANE, :].T
        top = jnp.max(m, axis=0, keepdims=True)
        mine_ref[j:j + 1, :] = top
        mine_ref[nb + j:nb + j + 1, :] = over_rows(s * jnp.exp2(m - top))
    copies = [send(mine_ref, box_ref.at[k], (s_sem, r_sem), k, peers[k]) for k in range(3)]

    lane = lax.broadcasted_iota(jnp.int32, (1, LANE), 1)
    edge = lane * LB + tp * vocab_local
    look_ref[ALL] = jnp.zeros_like(look_ref)
    steps = jnp.zeros((1, LANE), F32)
    for q in range(4):
        lo = jnp.zeros((1, LANE), F32)
        hi = jnp.zeros((1, LANE), F32)
        who = dp if q == 0 else xor(dp, q)
        for j in range(seq // LANE):
            ids = columns(all_ref[who, 2:3, LANE * j:LANE * j + LANE])
            lo = lo + over_rows(jnp.where(ids < edge, 1.0, 0.0))
            hi = hi + over_rows(jnp.where(ids < edge + LB, 1.0, 0.0))
        a = jnp.floor(lo * (1.0 / ST)) * ST
        look_ref[q:q + 1, :] = a.astype(jnp.int32)
        steps = jnp.maximum(steps, jnp.floor((hi - a + (CH - 1)) * (1.0 / CH)))
    look_ref[4:5, :] = steps.astype(jnp.int32)

    total = sum(over_lanes(all_ref[q, 1:2, :].astype(F32)) for q in range(4))
    shift = jnp.log(total) * LOG2E
    base = tp * vocab_local + core * (vocab_local // 2)
    half = nb // 2
    for c, out in ((chip, t_ref), (1 - chip, f_ref)):
        for j in range(nb):
            q, o = c * 2 + j // half, LANE * (j % half)
            on = all_ref[q, 1:2, o:o + LANE] > 0
            out[j:j + 1, :] = jnp.where(on, all_ref[q, 0:1, o:o + LANE] - base, -MIB)
    for copy in copies:
        copy.wait()
    parts = [mine_ref] + [box_ref.at[k] for k in range(3)]
    ms = [p[0:nb, :] for p in parts]
    top = functools.reduce(jnp.maximum, ms)
    w = [p[nb:2 * nb, :] * jnp.exp2(m - top) for p, m in zip(parts, ms)]
    lse = top + jnp.log((w[0] + w[1]) + (w[2] + w[3])) * LOG2E
    live = t_ref[ALL] > 1 - MIB
    k_ref[ALL] = jnp.where(live, lse + shift, jnp.inf)
    lse_ref[ALL] = jnp.broadcast_to(over_rows(jnp.where(live, lse, 0.0)), lse_ref.shape)


def final_kernel(a_ref, b_ref, h_ref, g_ref, on_ref, tl_ref, lse_ref, inv_ref, dh_ref, dg_ref, loss_ref, mine_ref, box_ref, s_sem, r_sem):
    dp, tp = lax.axis_index("dp"), lax.axis_index("tp")
    dps = [dp, xor(dp, 1), xor(dp, 2), xor(dp, 3)]
    peers = [(t, i) for t in (tp, 1 - tp) for i in dps][1:]
    greet(peers)
    d, seq = h_ref.shape
    x = h_ref[ALL].astype(F32)
    inv = lax.rsqrt(mean_rows(x * x) + RMS_EPS)
    u = x * inv
    dz = jnp.where(on_ref[ALL] > 0, a_ref[ALL] + b_ref[ALL], 0.0)
    prod = dz * u
    part = sum(prod[:, LANE * j:LANE * j + LANE] for j in range(seq // LANE))
    mine_ref[ALL] = jnp.zeros_like(mine_ref)
    mine_ref[0:1, 0:d] = over_rows(part.T)
    mine_ref[1:2, 0:LANE] = over_rows(tl_ref[ALL])
    mine_ref[2:3, 0:LANE] = lse_ref[0:1, :]
    box_ref[0] = mine_ref[ALL]
    copies = [send(mine_ref, box_ref.at[k + 1], (s_sem, r_sem), k, peers[k]) for k in range(7)]
    gain = jnp.concatenate([jnp.broadcast_to(g_ref[ALL].astype(F32)[None], (LANE, d)).T] * (seq // LANE), axis=1)
    w = dz * gain
    dh_ref[ALL] = (inv * (w - u * mean_rows(w * u))).astype(BF16)
    for copy in copies:
        copy.wait()
    same = [jnp.zeros((1, d), F32)] * 4
    found = jnp.zeros((1, LANE), F32)
    for q in range(4):
        row = jnp.zeros((1, d), F32)
        hit = jnp.zeros((1, LANE), F32)
        low = jnp.zeros((1, LANE), F32)
        for k in range(4):
            row = jnp.where(dps[k] == q, box_ref[k, 0:1, 0:d], row)
            hit = jnp.where(dps[k] == q, box_ref[k, 1:2, 0:LANE], hit)
            low = jnp.where(dps[k] == q, box_ref[k + 4, 1:2, 0:LANE], low)
        same[q] = row
        found = found + (hit + low)
    dg_ref[ALL] = (same[0] + same[1] + same[2] + same[3])[0]
    loss = over_lanes(box_ref[0, 2:3, 0:LANE] + box_ref[2, 2:3, 0:LANE] - found) * LN2
    loss_ref[ALL] = jnp.broadcast_to(loss, loss_ref.shape) * inv_ref[0:1, :]


def lookup_kernel(top, sc, look, from_ref, g1, g2, g3, g4, all_ref, *rest):
    out_ref, id_ref, row_ref = rest[-3:]
    b = pl.program_id(0)
    seq = all_ref.shape[2]
    lists = (g1, g2, g3, g4)

    @pl.when(b == 0)
    def _():
        for q, g in enumerate(lists):
            who = sc[2, 1] if q == 0 else xor(sc[2, 1], q)
            for j in range(seq // LANE):
                id_ref[q, LANE * j:LANE * j + LANE, :] = columns(all_ref[who, 2:3, LANE * j:LANE * j + LANE]) - sc[2, 5]
            row_ref[q, 0:seq, :] = g[ALL].astype(BF16).T
            id_ref[q, seq:, :] = jnp.full((CH, LANE), -MIB, jnp.int32)
            row_ref[q, seq:, :] = jnp.zeros((CH, row_ref.shape[2]), BF16)

    lane = lax.broadcasted_iota(jnp.int32, (CH, LB), 1)
    subs = from_ref.shape[1] // LB

    def part(at, k):
        hots, rows = [], []
        for q in range(len(lists)):
            c = pl.ds(pl.multiple_of(jnp.minimum(look[q, at] + k * CH, seq), ST), CH)
            ids = jnp.concatenate([id_ref[q, c, :] - at * LB] * (LB // LANE), axis=1)
            hots.append(jnp.where(ids == lane, 1.0, 0.0).astype(BF16))
            rows.append(row_ref[q, c, :])
        return lax.dot_general(
            jnp.concatenate(rows, axis=0), jnp.concatenate(hots, axis=0), (((0,), (0,)), ((), ())), preferred_element_type=F32)

    for u in range(subs):
        q = slice(u * LB, (u + 1) * LB)
        out_ref[:, q] = from_ref[:, q] + part(top(sc, b) * subs + u, 0)
    for u in range(subs):
        at = top(sc, b) * subs + u
        q = slice(u * LB, (u + 1) * LB)

        def step(k, _, at=at, q=q):
            out_ref[:, q] += part(at, k)
            return 0

        lax.fori_loop(1, look[4, at], step, 0)


def solution(mesh):
    n_dp = mesh.shape["dp"]
    swap = {k: [(i, i ^ k) for i in range(n_dp)] for k in (1, 2, 3)}

    def blocks(*arrays):
        return [pl.BlockSpec(a.shape, lambda i, n=len(a.shape): (0,) * n) for a in arrays]

    shape = jax.ShapeDtypeStruct

    def single(kernel, args, outs, scratch, ident=None):
        talk = {} if ident is None else dict(collective_id=ident, has_side_effects=True)
        return pl.pallas_call(
            kernel, grid=(1,), in_specs=blocks(*args), out_specs=blocks(*outs), out_shape=outs, scratch_shapes=scratch,
            compiler_params=pltpu.CompilerParams(dimension_semantics=("arbitrary",), vmem_limit_bytes=GRANT, **talk),
            cost_estimate=cost(SMALL))(*args)

    dma = pltpu.SemaphoreType.DMA

    def local_step(hidden, norm_w, embed, targets, loss_mask, token_ids, grad_embed):
        _, seq, d = hidden.shape
        vocab_local = embed.shape[0]
        half = vocab_local // 2
        nv = half // VB
        cols = d // n_dp
        nt = 2 * seq // TB
        et = embed.T
        ht = hidden[0].T

        zt32, zt_chip, z_chip, metas, table, inv_n, *give = single(
            functools.partial(prep_kernel, vocab_local),
            (ht, norm_w, targets, loss_mask, token_ids, grad_embed[0].T),
            [shape((d, seq), F32), shape((d, 2 * seq), BF16), shape((2 * seq, d), BF16),
             shape((n_dp, 8, seq), jnp.int32), shape((8, LANE), jnp.int32), shape((8, LANE), F32)] + [shape((cols, seq), F32)] * 4,
            [pltpu.VMEM((8, seq), jnp.int32), pltpu.VMEM((8, seq), jnp.int32),
             pltpu.VMEM((seq, LANE), jnp.int32), pltpu.VMEM((seq, seq), BF16), pltpu.VMEM((d, seq), F32),
             pltpu.VMEM((d, seq), F32), pltpu.VMEM((3, 8, seq), jnp.int32), pltpu.VMEM((3, 8, seq), jnp.int32),
             dma((7,)), dma((7,))], 0)

        far = lax.ppermute(zt32, "dp", swap[2])
        far_near = lax.ppermute(far, "dp", swap[1])

        def swap_call(own, give, a, b):
            w = 2 * seq // 8
            return pl.pallas_call(
                swap_kernel, grid=(8,),
                in_specs=[pl.BlockSpec((d, seq), lambda i: (0, 0)), pl.BlockSpec(memory_space=pl.ANY),
                          pl.BlockSpec((d, w), lambda i: (0, jnp.minimum(i, 3))), pl.BlockSpec((d, w), lambda i: (0, jnp.maximum(i - 4, 0)))],
                out_specs=[pl.BlockSpec((d, w), lambda i: (0, i)), pl.BlockSpec((w, d), lambda i: (i, 0)), pl.BlockSpec((d, seq), lambda i: (0, 0))],
                out_shape=[shape((d, 2 * seq), BF16), shape((2 * seq, d), BF16), shape((d, seq), F32)],
                scratch_shapes=[pltpu.VMEM((d, seq), F32), dma((1,)), dma((1,))],
                compiler_params=pltpu.CompilerParams(
                    dimension_semantics=("arbitrary",), vmem_limit_bytes=GRANT, collective_id=3, has_side_effects=True),
                name="swap", cost_estimate=cost(SMALL))(own, give, a, b)

        def specs(r):
            at = lambda x, t: lax.bitwise_xor(x[r, t], x[2, 0] * (nt // 2)) if r else x[r, t]
            full = lambda v, t, x: (0, 0)
            return dict(
                e=pl.BlockSpec((d, VB), lambda v, t, x: (0, x[2, 0] * nv + v)),
                z=pl.BlockSpec((TB, d), lambda v, t, x: (at(x, t), 0)),
                l=pl.BlockSpec((1, 1, TB, VB), lambda v, t, x: (x[r, t], v, 0, 0)),
                vec=pl.BlockSpec((2 * seq, LANE), full),
                row=pl.BlockSpec((2 * seq // LANE, LANE), full),
                any=pl.BlockSpec(memory_space=pl.ANY),
                inv=pl.BlockSpec((8, LANE), full),
                za=pl.BlockSpec((cols, TB), lambda v, t, x: (x[2, 1], at(x, t))),
                zb=pl.BlockSpec((cols, TB), lambda v, t, x: (x[2, 2], at(x, t))),
                de=pl.BlockSpec((cols, VB), lambda v, t, x: (0, v)))

        pick = lambda sp, *names: [sp[k] for k in names]
        own, other = specs(0), specs(1)
        vec = shape((2 * seq, LANE), F32)
        wide = [pltpu.VMEM((2 * seq, LANE), F32), pltpu.VMEM((2 * seq, LANE), jnp.int32)]
        de_shape = shape((cols, half), F32)
        flops = 2 * 2 * seq * half * d

        l_own, m_own, s_own = pl.pallas_call(
            logits_kernel,
            grid_spec=pltpu.PrefetchScalarGridSpec(
                num_scalar_prefetch=1, grid=(nv, nt), in_specs=pick(own, "z", "e"), out_specs=pick(own, "l", "vec", "vec")),
            out_shape=[shape((nt, nv, TB, VB), F32), vec, vec],
            compiler_params=params(), name="logits",
            cost_estimate=cost(flops),
        )(table, z_chip, et)

        rows = 2 * seq // LANE
        k_own, t_own, t_far, lse_sum, look = single(
            functools.partial(stats_kernel, vocab_local), (m_own, s_own, metas),
            [shape((rows, LANE), F32), shape((rows, LANE), jnp.int32), shape((rows, LANE), jnp.int32),
             shape((8, LANE), F32), shape((8, LANE), jnp.int32)],
            [pltpu.VMEM((2 * rows, LANE), F32), pltpu.VMEM((3, 2 * rows, LANE), F32), dma((3,)), dma((3,))], 1)
        k_far = lax.ppermute(k_own, "dp", swap[2])

        lists = [give[0]]
        for k in (1, 2, 3):
            lists.append(lax.ppermute(give[k], "dp", swap[k]))

        dz_own, dz_give, da, db, tl = pl.pallas_call(
            own_kernel,
            grid_spec=pltpu.PrefetchScalarGridSpec(
                num_scalar_prefetch=1, grid=(nv, nt),
                in_specs=pick(own, "l", "e", "za", "zb", "row", "row", "inv"), out_specs=pick(own, "any", "any", "de", "de", "vec"),
                scratch_shapes=[pltpu.VMEM((TB, VB), BF16), *wide, pltpu.VMEM((2, d, seq), F32), dma((2,))]),
            out_shape=[shape((d, seq), F32), shape((d, seq), F32), de_shape, de_shape, vec],
            compiler_params=params(), name="own",
            cost_estimate=cost(flops + flops // 2),
        )(table, l_own, et, zt_chip, zt_chip, k_own, t_own, inv_n)

        zt_far, z_far, dz_half = swap_call(dz_own, dz_give, far, far_near)
        dz_tp = lax.ppermute(dz_half, "tp", [(0, 1), (1, 0)])

        da, db = pl.pallas_call(
            other_kernel,
            grid_spec=pltpu.PrefetchScalarGridSpec(
                num_scalar_prefetch=1, grid=(nv, nt),
                in_specs=pick(other, "z", "e", "za", "zb", "row", "row", "inv", "de", "de"), out_specs=pick(other, "de", "de"),
                scratch_shapes=[pltpu.VMEM((TB, VB), F32), pltpu.VMEM((TB, VB), BF16), *wide]),
            out_shape=[de_shape, de_shape],
            compiler_params=params(), name="other",
            cost_estimate=cost(flops + flops // 2),
        )(table, z_far, et, zt_far, zt_far, k_far, t_far, inv_n, da, db)
        got = lax.ppermute(db, "dp", swap[1])

        nb = half // LW

        def lookup(top, source, *prior):
            zero = lambda b, x, k: (0, 0)
            return pl.pallas_call(
                functools.partial(lookup_kernel, top),
                grid_spec=pltpu.PrefetchScalarGridSpec(
                    num_scalar_prefetch=2, grid=(nb,),
                    in_specs=[pl.BlockSpec((cols, LW), lambda b, x, k: (0, b))] + [pl.BlockSpec((cols, seq), zero)] * 4
                    + [pl.BlockSpec((n_dp, 8, seq), lambda b, x, k: (0, 0, 0))] + [pl.BlockSpec(memory_space=pl.ANY)] * len(prior),
                    out_specs=pl.BlockSpec((cols, LW), lambda b, x, k: (0, top(x, b))),
                    scratch_shapes=[pltpu.VMEM((4, seq + CH, LANE), jnp.int32), pltpu.VMEM((4, seq + CH, cols), BF16)]),
                out_shape=shape((cols, vocab_local), F32),
                input_output_aliases={8: 0} if prior else {},
                compiler_params=params(1), name="lookup",
                cost_estimate=cost(flops // 8),
            )(table, look, source, *lists, metas, *prior)

        de_t = lookup(lambda x, b: x[2, 0] * nb + b, da)

        dht, dg, loss = single(
            final_kernel, (dz_half, dz_tp, ht, norm_w, loss_mask, tl, lse_sum, inv_n),
            [shape((d, seq), BF16), shape((d,), F32), shape((1, LANE), F32)],
            [pltpu.VMEM((8, 640), F32), pltpu.VMEM((8, 8, 640), F32), dma((7,)), dma((7,))], 2)

        de_t = lookup(lambda x, b: (1 - x[2, 0]) * nb + b, got, de_t)
        return loss[0, 0], dht.T[None], dg, de_t.T

    return jax.shard_map(
        local_step, mesh=mesh,
        in_specs=(P("dp"), P(), P("tp"), P("dp"), P("dp"), P("dp"), P("dp")),
        out_specs=(P(), P("dp"), P(), P("tp", "dp")), check_vma=False)
```

```python
import functools

import jax
import jax.numpy as jnp
from jax import lax
from jax.experimental import pallas as pl
from jax.experimental.pallas import tpu as pltpu
from jax.sharding import PartitionSpec as P


RMS_EPS = 1e-6
LOG2E = 1.4426950408889634
LN2 = 0.6931471805599453
TB = 256
VB = 6144
SC = 512
SF = 1024
LW = 6144
LB = 1024
CH = 128
ST = 16
LANE = 128
ALL = Ellipsis
MIB = 2**20
SMALL = 2**28
GRANT = 60 * 1024 * 1024
F32 = jnp.float32
BF16 = jnp.bfloat16


def over_lanes(x):
    return jnp.sum(x, axis=1, keepdims=True)


def over_rows(x):
    return jnp.sum(x, axis=0, keepdims=True)


def mean_rows(x):
    return jnp.mean(x, axis=0, keepdims=True)


def cost(flops):
    return pl.CostEstimate(flops=int(flops), bytes_accessed=MIB, transcendentals=0)


def params(n=2):
    return pltpu.CompilerParams(dimension_semantics=("arbitrary",) * n, vmem_limit_bytes=GRANT)


def stats_stage(l_ref, m_ref, s_ref, bases, c):
    for r in range(TB // 8):
        h, o = divmod(8 * r, LANE)
        rows = pl.ds(bases[h] + o, 8)
        old = m_ref[rows, :]
        total = s_ref[rows, :]
        parts = [l_ref[0, 0, 8 * r:8 * r + 8, c * SC + LANE * j:c * SC + LANE * j + LANE] for j in range(SC // LANE)]
        new = functools.reduce(jnp.maximum, parts, old)
        total = total * jnp.exp2(old - new)
        for part in parts:
            total = total + jnp.exp2(part - new)
        m_ref[rows, :] = new
        s_ref[rows, :] = total


def spots(sc, i):
    t = pl.program_id(1)
    return [pl.multiple_of(sc[i + h, t] * LANE, LANE) for h in range(TB // LANE)]


def logits_kernel(sc, z0, z1, e_ref, l_ref, m_ref, s_ref):
    v, t = pl.program_id(0), pl.program_id(1)
    bases = spots(sc, 0)
    skip = sc[4, 3]

    @pl.when((v == 0) & (t >= skip))
    def _():
        for base in bases:
            m_ref[pl.ds(base, LANE), :] = jnp.full((LANE, LANE), -3e38, F32)
            s_ref[pl.ds(base, LANE), :] = jnp.zeros((LANE, LANE), F32)

    @pl.when(t >= skip)
    def _():
        z = jnp.concatenate([z0[ALL], z1[ALL]], axis=0)
        n = VB // SC
        for c in range(n + 1):
            if c < n:
                q = slice(c * SC, (c + 1) * SC)
                l_ref[0, 0, :, q] = jnp.dot(z, e_ref[:, q], preferred_element_type=F32) * LOG2E
            if c > 0:
                stats_stage(l_ref, m_ref, s_ref, bases, c - 1)


def dlogits_stage(get, dl_ref, k_ref, scale, t_ref, tl_ref, bases, base, c, width):
    for r in range(TB // 16):
        h, o = divmod(16 * r, LANE)
        rows = pl.ds(bases[h] + o, 16)
        shift = k_ref[rows, :]
        target = t_ref[rows, :] - base
        if tl_ref is not None:
            found = tl_ref[rows, :]
        for j in range(width // LANE):
            o = c * width + LANE * j
            x = get(r, o)
            hit = target == o
            p = jnp.exp2(x - shift)
            if tl_ref is not None:
                found = jnp.where(hit, x, found)
            dl_ref[16 * r:16 * r + 16, o:o + LANE] = jnp.where(hit, p - scale, p).astype(BF16)
        if tl_ref is not None:
            tl_ref[rows, :] = found


def pair_columns(a, b, c, d):
    return jnp.concatenate([jnp.concatenate([a[ALL], b[ALL]], axis=1), jnp.concatenate([c[ALL], d[ALL]], axis=1)], axis=0)


def own_kernel(sc, l_ref, e_ref, za0, za1, zb0, zb1, k_ref, t_ref, inv_ref, dz_ref, gv_ref, da_ref, db_ref, tl_ref, dl_ref, kw_ref, tw_ref, part_ref, acc_ref, sem):
    v, t = pl.program_id(0), pl.program_id(1)
    bases = spots(sc, 0)
    skip = sc[4, 3]

    expand(t, v, skip, bases, k_ref, t_ref, kw_ref, tw_ref)
    seq = acc_ref.shape[2]
    slots = [lax.bitwise_xor(lax.div(base, seq), sc[4, 0]) for base in bases]
    places = [pl.ds(pl.multiple_of(lax.rem(base, seq), LANE), LANE) for base in bases]

    @pl.when((v == 0) & (t >= skip))
    def _():
        for slot, place in zip(slots, places):
            acc_ref[slot, :, place] = jnp.zeros((acc_ref.shape[1], LANE), F32)

    @pl.when((v == 0) & (t == 0))
    def _():
        tl_ref[ALL] = jnp.zeros_like(tl_ref)

    @pl.when(t == skip)
    def _():
        da_ref[ALL] = jnp.zeros_like(da_ref)
        db_ref[ALL] = jnp.zeros_like(db_ref)

    @pl.when(t >= skip)
    def _():
        zc = pair_columns(za0, za1, zb0, zb1)
        half = za0.shape[0]
        scale = jnp.concatenate([inv_ref[ALL], inv_ref[ALL]], axis=0)
        n = VB // SC
        get = lambda r, o: l_ref[0, 0, 16 * r:16 * r + 16, o:o + LANE]
        for c in range(n + 1):
            if c < n:
                dlogits_stage(get, dl_ref, kw_ref, scale, tw_ref, tl_ref, bases, v * VB, c, SC)
            if c > 0:
                q = slice((c - 1) * SC, c * SC)
                dl = dl_ref[:, q]
                dz = lax.dot_general(e_ref[:, q], dl, (((1,), (1,)), ((), ())), preferred_element_type=F32)
                part_ref[ALL] = dz if c == 1 else part_ref[ALL] + dz
                de = jnp.dot(zc, dl, preferred_element_type=F32)
                da_ref[:, q] += de[:half]
                db_ref[:, q] += de[half:]
        for h, (slot, place) in enumerate(zip(slots, places)):
            acc_ref[slot, :, place] += part_ref[:, LANE * h:LANE * h + LANE]

    @pl.when((v == pl.num_programs(0) - 1) & (t == pl.num_programs(1) - 1))
    def _():
        copies = [pltpu.make_async_copy(acc_ref.at[k], out, sem.at[k]) for k, out in enumerate((dz_ref, gv_ref))]
        for copy in copies:
            copy.start()
        for copy in copies:
            copy.wait()


def other_kernel(sc, z0, z1, e_ref, za0, za1, zb0, zb1, k_ref, t_ref, inv_ref, ia_ref, ib_ref, da_ref, db_ref, l_ref, dl_ref, kw_ref, tw_ref):
    v, t = pl.program_id(0), pl.program_id(1)
    bases = spots(sc, 2)
    skip = sc[4, 4]
    expand(t, v, skip, bases, k_ref, t_ref, kw_ref, tw_ref)

    @pl.when(t == skip)
    def _():
        da_ref[ALL] = ia_ref[ALL]
        db_ref[ALL] = ib_ref[ALL]

    @pl.when(t >= skip)
    def _():
        zc = pair_columns(za0, za1, zb0, zb1)
        half = za0.shape[0]
        z = jnp.concatenate([z0[ALL], z1[ALL]], axis=0)
        scale = jnp.concatenate([inv_ref[ALL], inv_ref[ALL]], axis=0)
        n = VB // SF
        get = lambda r, o: l_ref[16 * r:16 * r + 16, o:o + LANE] * LOG2E
        for c in range(n + 2):
            if c < n:
                q = slice(c * SF, (c + 1) * SF)
                l_ref[:, q] = jnp.dot(z, e_ref[:, q], preferred_element_type=F32)
            if 0 < c <= n:
                dlogits_stage(get, dl_ref, kw_ref, scale, tw_ref, None, bases, v * VB, c - 1, SF)
            if c > 1:
                q = slice((c - 2) * SF, (c - 1) * SF)
                de = jnp.dot(zc, dl_ref[:, q], preferred_element_type=F32)
                da_ref[:, q] += de[:half]
                db_ref[:, q] += de[half:]


def swap_kernel(own_ref, give_ref, a_ref, b_ref, zt_ref, z_ref, dz_ref, got_ref, s_sem, r_sem):
    dp, tp = lax.axis_index("dp"), lax.axis_index("tp")
    i, n = pl.program_id(0), pl.num_programs(0)
    peer = (tp, xor(dp, 1))
    copy = link(give_ref, got_ref, (s_sem, r_sem), 0, peer)

    @pl.when(i == 0)
    def _():
        greet([peer])
        copy.start()

    z = jnp.where(i < 4, a_ref[ALL], b_ref[ALL]).astype(BF16)
    zt_ref[ALL] = z
    z_ref[ALL] = z.T

    @pl.when(i == n - 1)
    def _():
        copy.wait()
        dz_ref[ALL] = own_ref[ALL] + got_ref[ALL]


def xor(i, k):
    return (i + 1 - 2 * lax.rem(i, 2), lax.rem(i + 2, 4), 3 - i)[k - 1]


def expand(t, v, skip, bases, k_ref, t_ref, kw_ref, tw_ref):
    @pl.when((v == 0) & (t >= skip))
    def _():
        lane = lax.broadcasted_iota(jnp.int32, (1, LANE), 1)
        for base in bases:
            r = pl.ds(lax.div(base, LANE), 1)
            kw_ref[pl.ds(base, LANE), :] = columns(k_ref[r, :])
            tw_ref[pl.ds(base, LANE), :] = columns(t_ref[r, :]) - lane


def columns(row):
    return jnp.broadcast_to(row, (LANE, LANE)).T


def sort_lists(i_ref, ge_ref, outs, ids_ref, key_ref, perm_ref, sorted_ref):
    seq = i_ref.shape[1]
    nb = seq // LANE
    lane = lax.broadcasted_iota(jnp.int32, (1, LANE), 1)
    rows = [i_ref[:, LANE * j:LANE * j + LANE] * seq + lane + LANE * j for j in range(nb)]
    for j in range(nb):
        key_ref[LANE * j:LANE * j + LANE, :] = columns(rows[j])
    keys = key_ref[ALL]
    before = jnp.zeros((seq, LANE), F32)
    for j in range(nb):
        before = before + jnp.where(rows[j] < keys, 1.0, 0.0)
    rank = jnp.broadcast_to(over_lanes(before), (seq, LANE)).astype(jnp.int32)
    ids_ref[ALL] = jnp.zeros_like(ids_ref)
    for j in range(nb):
        hit = rank == lane + LANE * j
        perm_ref[:, LANE * j:LANE * j + LANE] = jnp.where(hit, 1.0, 0.0).astype(BF16)
        place = over_rows(jnp.where(hit, keys, 0))
        ids_ref[0:1, LANE * j:LANE * j + LANE] = lax.shift_right_logical(place, seq.bit_length() - 1)
    sorted_ref[ALL] = jnp.dot(ge_ref[ALL], perm_ref[ALL], preferred_element_type=F32)
    dp = lax.axis_index("dp")
    cols = outs[0].shape[0]
    for k, o in enumerate(outs):
        who = dp if k == 0 else xor(dp, k)
        o[ALL] = sorted_ref[pl.ds(pl.multiple_of(who * cols, 8), cols), :]


def greet(peers):
    barrier = pltpu.get_barrier_semaphore()
    for peer in peers:
        pl.semaphore_signal(barrier, inc=1, device_id=peer, device_id_type=pl.DeviceIdType.MESH)
    pl.semaphore_wait(barrier, len(peers))


def send(src, dst, sems, k, peer):
    copy = link(src, dst, sems, k, peer)
    copy.start()
    return copy


def link(src, dst, sems, k, peer):
    return pltpu.make_async_remote_copy(
        src_ref=src, dst_ref=dst, send_sem=sems[0].at[k], recv_sem=sems[1].at[k],
        device_id=peer, device_id_type=pl.DeviceIdType.MESH)


def prep_kernel(vocab_local, h_ref, g_ref, t_ref, m_ref, i_ref, ge_ref, z32_ref, zt_ref, z_ref, all_ref, table_ref, inv_ref, o1, o2, o3, o4,
                meta_ref, ids_ref, key_ref, perm_ref, sorted_ref, got_ref, box_ref, id_box_ref, s_sem, r_sem):
    dp, tp = lax.axis_index("dp"), lax.axis_index("tp")
    core = lax.rem(dp, 2)
    chip = lax.div(dp, 2)
    d, seq = h_ref.shape
    at = lambda i: (tp, i)
    peers = [at(xor(dp, k)) for k in (1, 2, 3)]
    meta_ref[ALL] = jnp.zeros_like(meta_ref)
    meta_ref[0:1, :] = t_ref[ALL]
    meta_ref[1:2, :] = m_ref[ALL]
    greet(peers)
    sems = (s_sem, r_sem)
    copies = [send(meta_ref, box_ref.at[k], sems, k, peers[k]) for k in range(3)]
    x = h_ref[ALL].astype(F32)
    inv = lax.rsqrt(mean_rows(x * x) + RMS_EPS)
    gain = jnp.concatenate([jnp.broadcast_to(g_ref[ALL].astype(F32)[None], (LANE, d)).T] * (seq // LANE), axis=1)
    z = (x * inv * gain).astype(BF16)
    z32_ref[ALL] = z.astype(F32)
    z_ref[pl.ds(pl.multiple_of(core * seq, seq), seq), :] = z.T
    copies.append(send(z32_ref, got_ref, sems, 3, peers[0]))
    zt_ref[:, pl.ds(pl.multiple_of(core * seq, seq), seq)] = z
    sort_lists(i_ref, ge_ref, (o1, o2, o3, o4), ids_ref, key_ref, perm_ref, sorted_ref)
    id_copies = [send(ids_ref, id_box_ref.at[k], sems, k + 4, peers[k]) for k in range(3)]
    for copy in copies[:3]:
        copy.wait()
    all_ref[dp] = meta_ref[ALL]
    for k in range(3):
        all_ref[xor(dp, k + 1)] = box_ref[k]

    tiles = []
    total = jnp.zeros((1, 1), F32)
    for q in range(4):
        length = over_lanes(all_ref[q, 1:2, :].astype(F32))
        total = total + length
        tiles.append(jnp.floor((length + (LANE - 1)) * (1.0 / LANE)).astype(jnp.int32))
    inv_ref[ALL] = jnp.broadcast_to(1.0 / total, inv_ref.shape)
    nt = 2 * seq // TB
    lane = lax.broadcasted_iota(jnp.int32, (1, LANE), 1)
    swap = chip == 1
    pairs = [(tiles[0], tiles[1]), (tiles[2], tiles[3])]
    out = []
    skips = []
    for c in range(2):
        na = jnp.where(swap, pairs[1 - c][0], pairs[c][0])
        nb = jnp.where(swap, pairs[1 - c][1], pairs[c][1])
        skip = nt - lax.shift_right_logical(na + nb + 1, 1)
        full = seq // LANE
        spare = jnp.minimum(jnp.where(na < full, na, full + nb), 2 * full - 1)
        for h in range(TB // LANE):
            p = 2 * jnp.maximum(lane - skip, 0) + h
            out.append(jnp.where(p < na, p, jnp.where(p < na + nb, full + p - na, spare)))
        skips.append(skip)
    row = jnp.where(lane == 0, core, jnp.where(lane == 1, dp, jnp.where(lane == 2, xor(dp, 1), jnp.where(lane == 3, skips[0], jnp.where(lane == 4, skips[1], tp * vocab_local)))))
    table_ref[ALL] = jnp.zeros_like(table_ref)
    for k, line in enumerate(out + [row]):
        table_ref[k:k + 1, :] = line

    copies[3].wait()
    other = xor(dp, 1) - 2 * chip
    got = got_ref[ALL].astype(BF16)
    z_ref[pl.ds(pl.multiple_of(other * seq, seq), seq), :] = got.T
    zt_ref[:, pl.ds(pl.multiple_of(other * seq, seq), seq)] = got
    for copy in id_copies:
        copy.wait()
    all_ref[dp, 2:3, :] = ids_ref[0:1, :]
    for k in range(3):
        all_ref[xor(dp, k + 1), 2:3, :] = id_box_ref[k, 0:1, :]


def stats_kernel(vocab_local, m_ref, s_ref, all_ref, k_ref, t_ref, f_ref, lse_ref, look_ref, mine_ref, box_ref, s_sem, r_sem):
    dp, tp = lax.axis_index("dp"), lax.axis_index("tp")
    core = lax.rem(dp, 2)
    chip = lax.div(dp, 2)
    seq = all_ref.shape[2]
    nb = m_ref.shape[0] // LANE
    peers = [(tp, xor(dp, 1)), (1 - tp, dp), (1 - tp, xor(dp, 1))]
    greet(peers)
    for j in range(nb):
        m = m_ref[LANE * j:LANE * j + LANE, :].T
        s = s_ref[LANE * j:LANE * j + LANE, :].T
        top = jnp.max(m, axis=0, keepdims=True)
        mine_ref[j:j + 1, :] = top
        mine_ref[nb + j:nb + j + 1, :] = over_rows(s * jnp.exp2(m - top))
    copies = [send(mine_ref, box_ref.at[k], (s_sem, r_sem), k, peers[k]) for k in range(3)]

    lane = lax.broadcasted_iota(jnp.int32, (1, LANE), 1)
    edge = lane * LB + tp * vocab_local
    look_ref[ALL] = jnp.zeros_like(look_ref)
    steps = jnp.zeros((1, LANE), F32)
    for q in range(4):
        lo = jnp.zeros((1, LANE), F32)
        hi = jnp.zeros((1, LANE), F32)
        who = dp if q == 0 else xor(dp, q)
        for j in range(seq // LANE):
            ids = columns(all_ref[who, 2:3, LANE * j:LANE * j + LANE])
            lo = lo + over_rows(jnp.where(ids < edge, 1.0, 0.0))
            hi = hi + over_rows(jnp.where(ids < edge + LB, 1.0, 0.0))
        a = jnp.floor(lo * (1.0 / ST)) * ST
        look_ref[q:q + 1, :] = a.astype(jnp.int32)
        steps = jnp.maximum(steps, jnp.floor((hi - a + (CH - 1)) * (1.0 / CH)))
    look_ref[4:5, :] = steps.astype(jnp.int32)

    total = sum(over_lanes(all_ref[q, 1:2, :].astype(F32)) for q in range(4))
    shift = jnp.log(total) * LOG2E
    base = tp * vocab_local + core * (vocab_local // 2)
    half = nb // 2
    for c, out in ((chip, t_ref), (1 - chip, f_ref)):
        for j in range(nb):
            q, o = c * 2 + j // half, LANE * (j % half)
            on = all_ref[q, 1:2, o:o + LANE] > 0
            out[j:j + 1, :] = jnp.where(on, all_ref[q, 0:1, o:o + LANE] - base, -MIB)
    for copy in copies:
        copy.wait()
    parts = [mine_ref] + [box_ref.at[k] for k in range(3)]
    ms = [p[0:nb, :] for p in parts]
    top = functools.reduce(jnp.maximum, ms)
    w = [p[nb:2 * nb, :] * jnp.exp2(m - top) for p, m in zip(parts, ms)]
    lse = top + jnp.log((w[0] + w[1]) + (w[2] + w[3])) * LOG2E
    live = t_ref[ALL] > 1 - MIB
    k_ref[ALL] = jnp.where(live, lse + shift, jnp.inf)
    lse_ref[ALL] = jnp.broadcast_to(over_rows(jnp.where(live, lse, 0.0)), lse_ref.shape)


def final_kernel(a_ref, b_ref, h_ref, g_ref, on_ref, tl_ref, lse_ref, inv_ref, dh_ref, dg_ref, loss_ref, mine_ref, box_ref, s_sem, r_sem):
    dp, tp = lax.axis_index("dp"), lax.axis_index("tp")
    dps = [dp, xor(dp, 1), xor(dp, 2), xor(dp, 3)]
    peers = [(t, i) for t in (tp, 1 - tp) for i in dps][1:]
    greet(peers)
    d, seq = h_ref.shape
    x = h_ref[ALL].astype(F32)
    inv = lax.rsqrt(mean_rows(x * x) + RMS_EPS)
    u = x * inv
    dz = jnp.where(on_ref[ALL] > 0, a_ref[ALL] + b_ref[ALL], 0.0)
    prod = dz * u
    part = sum(prod[:, LANE * j:LANE * j + LANE] for j in range(seq // LANE))
    mine_ref[ALL] = jnp.zeros_like(mine_ref)
    mine_ref[0:1, 0:d] = over_rows(part.T)
    mine_ref[1:2, 0:LANE] = over_rows(tl_ref[ALL])
    mine_ref[2:3, 0:LANE] = lse_ref[0:1, :]
    box_ref[0] = mine_ref[ALL]
    copies = [send(mine_ref, box_ref.at[k + 1], (s_sem, r_sem), k, peers[k]) for k in range(7)]
    gain = jnp.concatenate([jnp.broadcast_to(g_ref[ALL].astype(F32)[None], (LANE, d)).T] * (seq // LANE), axis=1)
    w = dz * gain
    dh_ref[ALL] = (inv * (w - u * mean_rows(w * u))).astype(BF16)
    for copy in copies:
        copy.wait()
    same = [jnp.zeros((1, d), F32)] * 4
    found = jnp.zeros((1, LANE), F32)
    for q in range(4):
        row = jnp.zeros((1, d), F32)
        hit = jnp.zeros((1, LANE), F32)
        low = jnp.zeros((1, LANE), F32)
        for k in range(4):
            row = jnp.where(dps[k] == q, box_ref[k, 0:1, 0:d], row)
            hit = jnp.where(dps[k] == q, box_ref[k, 1:2, 0:LANE], hit)
            low = jnp.where(dps[k] == q, box_ref[k + 4, 1:2, 0:LANE], low)
        same[q] = row
        found = found + (hit + low)
    dg_ref[ALL] = (same[0] + same[1] + same[2] + same[3])[0]
    loss = over_lanes(box_ref[0, 2:3, 0:LANE] + box_ref[2, 2:3, 0:LANE] - found) * LN2
    loss_ref[ALL] = jnp.broadcast_to(loss, loss_ref.shape) * inv_ref[0:1, :]


def lookup_kernel(top, sc, look, from_ref, g1, g2, g3, g4, all_ref, *rest):
    out_ref, id_ref, row_ref = rest[-3:]
    b = pl.program_id(0)
    seq = all_ref.shape[2]
    lists = (g1, g2, g3, g4)

    @pl.when(b == 0)
    def _():
        for q, g in enumerate(lists):
            who = sc[4, 1] if q == 0 else xor(sc[4, 1], q)
            for j in range(seq // LANE):
                id_ref[q, LANE * j:LANE * j + LANE, :] = columns(all_ref[who, 2:3, LANE * j:LANE * j + LANE]) - sc[4, 5]
            row_ref[q, 0:seq, :] = g[ALL].astype(BF16).T
            id_ref[q, seq:, :] = jnp.full((CH, LANE), -MIB, jnp.int32)
            row_ref[q, seq:, :] = jnp.zeros((CH, row_ref.shape[2]), BF16)

    lane = lax.broadcasted_iota(jnp.int32, (CH, LB), 1)
    subs = from_ref.shape[1] // LB

    def part(at, k):
        hots, rows = [], []
        for q in range(len(lists)):
            c = pl.ds(pl.multiple_of(jnp.minimum(look[q, at] + k * CH, seq), ST), CH)
            ids = jnp.concatenate([id_ref[q, c, :] - at * LB] * (LB // LANE), axis=1)
            hots.append(jnp.where(ids == lane, 1.0, 0.0).astype(BF16))
            rows.append(row_ref[q, c, :])
        return lax.dot_general(
            jnp.concatenate(rows, axis=0), jnp.concatenate(hots, axis=0), (((0,), (0,)), ((), ())), preferred_element_type=F32)

    for u in range(subs):
        q = slice(u * LB, (u + 1) * LB)
        out_ref[:, q] = from_ref[:, q] + part(top(sc, b) * subs + u, 0)
    for u in range(subs):
        at = top(sc, b) * subs + u
        q = slice(u * LB, (u + 1) * LB)

        def step(k, _, at=at, q=q):
            out_ref[:, q] += part(at, k)
            return 0

        lax.fori_loop(1, look[4, at], step, 0)


def solution(mesh):
    n_dp = mesh.shape["dp"]
    swap = {k: [(i, i ^ k) for i in range(n_dp)] for k in (1, 2, 3)}

    def blocks(*arrays):
        return [pl.BlockSpec(a.shape, lambda i, n=len(a.shape): (0,) * n) for a in arrays]

    shape = jax.ShapeDtypeStruct

    def single(kernel, args, outs, scratch, ident=None):
        talk = {} if ident is None else dict(collective_id=ident, has_side_effects=True)
        return pl.pallas_call(
            kernel, grid=(1,), in_specs=blocks(*args), out_specs=blocks(*outs), out_shape=outs, scratch_shapes=scratch,
            compiler_params=pltpu.CompilerParams(dimension_semantics=("arbitrary",), vmem_limit_bytes=GRANT, **talk),
            cost_estimate=cost(SMALL))(*args)

    dma = pltpu.SemaphoreType.DMA

    def local_step(hidden, norm_w, embed, targets, loss_mask, token_ids, grad_embed):
        _, seq, d = hidden.shape
        vocab_local = embed.shape[0]
        half = vocab_local // 2
        nv = half // VB
        cols = d // n_dp
        nt = 2 * seq // TB
        et = embed.T
        ht = hidden[0].T

        zt32, zt_chip, z_chip, metas, table, inv_n, *give = single(
            functools.partial(prep_kernel, vocab_local),
            (ht, norm_w, targets, loss_mask, token_ids, grad_embed[0].T),
            [shape((d, seq), F32), shape((d, 2 * seq), BF16), shape((2 * seq, d), BF16),
             shape((n_dp, 8, seq), jnp.int32), shape((8, LANE), jnp.int32), shape((8, LANE), F32)] + [shape((cols, seq), F32)] * 4,
            [pltpu.VMEM((8, seq), jnp.int32), pltpu.VMEM((8, seq), jnp.int32),
             pltpu.VMEM((seq, LANE), jnp.int32), pltpu.VMEM((seq, seq), BF16), pltpu.VMEM((d, seq), F32),
             pltpu.VMEM((d, seq), F32), pltpu.VMEM((3, 8, seq), jnp.int32), pltpu.VMEM((3, 8, seq), jnp.int32),
             dma((7,)), dma((7,))], 0)

        far = lax.ppermute(zt32, "dp", swap[2])
        far_near = lax.ppermute(far, "dp", swap[1])

        def swap_call(own, give, a, b):
            w = 2 * seq // 8
            return pl.pallas_call(
                swap_kernel, grid=(8,),
                in_specs=[pl.BlockSpec((d, seq), lambda i: (0, 0)), pl.BlockSpec(memory_space=pl.ANY),
                          pl.BlockSpec((d, w), lambda i: (0, jnp.minimum(i, 3))), pl.BlockSpec((d, w), lambda i: (0, jnp.maximum(i - 4, 0)))],
                out_specs=[pl.BlockSpec((d, w), lambda i: (0, i)), pl.BlockSpec((w, d), lambda i: (i, 0)), pl.BlockSpec((d, seq), lambda i: (0, 0))],
                out_shape=[shape((d, 2 * seq), BF16), shape((2 * seq, d), BF16), shape((d, seq), F32)],
                scratch_shapes=[pltpu.VMEM((d, seq), F32), dma((1,)), dma((1,))],
                compiler_params=pltpu.CompilerParams(
                    dimension_semantics=("arbitrary",), vmem_limit_bytes=GRANT, collective_id=3, has_side_effects=True),
                name="swap", cost_estimate=cost(SMALL))(own, give, a, b)

        def specs(r):
            at = lambda x, t, h: lax.bitwise_xor(x[r + h, t], x[4, 0] * (seq // LANE)) if r else x[h, t]
            full = lambda v, t, x: (0, 0)
            halves = range(TB // LANE)
            return dict(
                e=[pl.BlockSpec((d, VB), lambda v, t, x: (0, x[4, 0] * nv + v))],
                z=[pl.BlockSpec((LANE, d), lambda v, t, x, h=h: (at(x, t, h), 0)) for h in halves],
                l=[pl.BlockSpec((1, 1, TB, VB), lambda v, t, x: (jnp.maximum(t, x[4, 3]), v, 0, 0))],
                vec=[pl.BlockSpec((2 * seq, LANE), full)],
                row=[pl.BlockSpec((2 * seq // LANE, LANE), full)],
                any=[pl.BlockSpec(memory_space=pl.ANY)],
                inv=[pl.BlockSpec((8, LANE), full)],
                zc=[pl.BlockSpec((cols, LANE), lambda v, t, x, h=h, k=k: (x[4, k], at(x, t, h))) for k in (1, 2) for h in halves],
                de=[pl.BlockSpec((cols, VB), lambda v, t, x: (0, v))])

        pick = lambda sp, *names: [b for k in names for b in sp[k]]
        own, other = specs(0), specs(2)
        vec = shape((2 * seq, LANE), F32)
        wide = [pltpu.VMEM((2 * seq, LANE), F32), pltpu.VMEM((2 * seq, LANE), jnp.int32)]
        de_shape = shape((cols, half), F32)
        flops = 2 * 2 * seq * half * d

        l_own, m_own, s_own = pl.pallas_call(
            logits_kernel,
            grid_spec=pltpu.PrefetchScalarGridSpec(
                num_scalar_prefetch=1, grid=(nv, nt), in_specs=pick(own, "z", "e"), out_specs=pick(own, "l", "vec", "vec")),
            out_shape=[shape((nt, nv, TB, VB), F32), vec, vec],
            compiler_params=params(), name="logits",
            cost_estimate=cost(flops),
        )(table, z_chip, z_chip, et)

        rows = 2 * seq // LANE
        k_own, t_own, t_far, lse_sum, look = single(
            functools.partial(stats_kernel, vocab_local), (m_own, s_own, metas),
            [shape((rows, LANE), F32), shape((rows, LANE), jnp.int32), shape((rows, LANE), jnp.int32),
             shape((8, LANE), F32), shape((8, LANE), jnp.int32)],
            [pltpu.VMEM((2 * rows, LANE), F32), pltpu.VMEM((3, 2 * rows, LANE), F32), dma((3,)), dma((3,))], 1)
        k_far = lax.ppermute(k_own, "dp", swap[2])

        lists = [give[0]]
        for k in (1, 2, 3):
            lists.append(lax.ppermute(give[k], "dp", swap[k]))

        dz_own, dz_give, da, db, tl = pl.pallas_call(
            own_kernel,
            grid_spec=pltpu.PrefetchScalarGridSpec(
                num_scalar_prefetch=1, grid=(nv, nt),
                in_specs=pick(own, "l", "e", "zc", "row", "row", "inv"), out_specs=pick(own, "any", "any", "de", "de", "vec"),
                scratch_shapes=[pltpu.VMEM((TB, VB), BF16), *wide, pltpu.VMEM((d, TB), F32), pltpu.VMEM((2, d, seq), F32), dma((2,))]),
            out_shape=[shape((d, seq), F32), shape((d, seq), F32), de_shape, de_shape, vec],
            compiler_params=params(), name="own",
            cost_estimate=cost(flops + flops // 2),
        )(table, l_own, et, *[zt_chip] * 4, k_own, t_own, inv_n)

        zt_far, z_far, dz_half = swap_call(dz_own, dz_give, far, far_near)
        dz_tp = lax.ppermute(dz_half, "tp", [(0, 1), (1, 0)])

        da, db = pl.pallas_call(
            other_kernel,
            grid_spec=pltpu.PrefetchScalarGridSpec(
                num_scalar_prefetch=1, grid=(nv, nt),
                in_specs=pick(other, "z", "e", "zc", "row", "row", "inv", "de", "de"), out_specs=pick(other, "de", "de"),
                scratch_shapes=[pltpu.VMEM((TB, VB), F32), pltpu.VMEM((TB, VB), BF16), *wide]),
            out_shape=[de_shape, de_shape],
            compiler_params=params(), name="other",
            cost_estimate=cost(flops + flops // 2),
        )(table, z_far, z_far, et, *[zt_far] * 4, k_far, t_far, inv_n, da, db)
        got = lax.ppermute(db, "dp", swap[1])

        nb = half // LW

        def lookup(top, source, *prior):
            zero = lambda b, x, k: (0, 0)
            return pl.pallas_call(
                functools.partial(lookup_kernel, top),
                grid_spec=pltpu.PrefetchScalarGridSpec(
                    num_scalar_prefetch=2, grid=(nb,),
                    in_specs=[pl.BlockSpec((cols, LW), lambda b, x, k: (0, b))] + [pl.BlockSpec((cols, seq), zero)] * 4
                    + [pl.BlockSpec((n_dp, 8, seq), lambda b, x, k: (0, 0, 0))] + [pl.BlockSpec(memory_space=pl.ANY)] * len(prior),
                    out_specs=pl.BlockSpec((cols, LW), lambda b, x, k: (0, top(x, b))),
                    scratch_shapes=[pltpu.VMEM((4, seq + CH, LANE), jnp.int32), pltpu.VMEM((4, seq + CH, cols), BF16)]),
                out_shape=shape((cols, vocab_local), F32),
                input_output_aliases={8: 0} if prior else {},
                compiler_params=params(1), name="lookup",
                cost_estimate=cost(flops // 8),
            )(table, look, source, *lists, metas, *prior)

        de_t = lookup(lambda x, b: x[4, 0] * nb + b, da)

        dht, dg, loss = single(
            final_kernel, (dz_half, dz_tp, ht, norm_w, loss_mask, tl, lse_sum, inv_n),
            [shape((d, seq), BF16), shape((d,), F32), shape((1, LANE), F32)],
            [pltpu.VMEM((8, 640), F32), pltpu.VMEM((8, 8, 640), F32), dma((7,)), dma((7,))], 2)

        de_t = lookup(lambda x, b: (1 - x[4, 0]) * nb + b, got, de_t)
        return loss[0, 0], dht.T[None], dg, de_t.T

    return jax.shard_map(
        local_step, mesh=mesh,
        in_specs=(P("dp"), P(), P("tp"), P("dp"), P("dp"), P("dp"), P("dp")),
        out_specs=(P(), P("dp"), P(), P("tp", "dp")), check_vma=False)
```

```python
import functools

import jax
import jax.numpy as jnp
from jax import lax
from jax.experimental import pallas as pl
from jax.experimental.pallas import tpu as pltpu
from jax.sharding import PartitionSpec as P


RMS_EPS = 1e-6
LOG2E = 1.4426950408889634
LN2 = 0.6931471805599453
TB = 256
VB = 6144
SC = 512
SF = 1024
LW = 6144
LB = 512
CH = 128
ST = 16
LANE = 128
ALL = Ellipsis
MIB = 2**20
SMALL = 2**28
GRANT = 60 * 1024 * 1024
F32 = jnp.float32
BF16 = jnp.bfloat16


def over_lanes(x):
    return jnp.sum(x, axis=1, keepdims=True)


def over_rows(x):
    return jnp.sum(x, axis=0, keepdims=True)


def mean_rows(x):
    return jnp.mean(x, axis=0, keepdims=True)


def cost(flops):
    return pl.CostEstimate(flops=int(flops), bytes_accessed=MIB, transcendentals=0)


def params(n=2):
    return pltpu.CompilerParams(dimension_semantics=("arbitrary",) * n, vmem_limit_bytes=GRANT)


def stats_stage(l_ref, m_ref, s_ref, bases, c):
    for r in range(TB // 8):
        h, o = divmod(8 * r, LANE)
        rows = pl.ds(bases[h] + o, 8)
        old = m_ref[rows, :]
        total = s_ref[rows, :]
        parts = [l_ref[0, 0, 8 * r:8 * r + 8, c * SC + LANE * j:c * SC + LANE * j + LANE] for j in range(SC // LANE)]
        new = functools.reduce(jnp.maximum, parts, old)
        total = total * jnp.exp2(old - new)
        for part in parts:
            total = total + jnp.exp2(part - new)
        m_ref[rows, :] = new
        s_ref[rows, :] = total


def spots(sc, i):
    t = pl.program_id(1)
    return [pl.multiple_of(sc[i + h, t] * LANE, LANE) for h in range(TB // LANE)]


def logits_kernel(sc, z0, z1, e_ref, l_ref, m_ref, s_ref):
    v, t = pl.program_id(0), pl.program_id(1)
    bases = spots(sc, 0)
    skip = sc[4, 3]

    @pl.when((v == 0) & (t >= skip))
    def _():
        for base in bases:
            m_ref[pl.ds(base, LANE), :] = jnp.full((LANE, LANE), -3e38, F32)
            s_ref[pl.ds(base, LANE), :] = jnp.zeros((LANE, LANE), F32)

    @pl.when(t >= skip)
    def _():
        z = jnp.concatenate([z0[ALL], z1[ALL]], axis=0)
        n = VB // SC
        for c in range(n + 1):
            if c < n:
                q = slice(c * SC, (c + 1) * SC)
                l_ref[0, 0, :, q] = jnp.dot(z, e_ref[:, q], preferred_element_type=F32) * LOG2E
            if c > 0:
                stats_stage(l_ref, m_ref, s_ref, bases, c - 1)


def dlogits_stage(get, dl_ref, k_ref, scale, t_ref, tl_ref, bases, base, c, width):
    for r in range(TB // 16):
        h, o = divmod(16 * r, LANE)
        rows = pl.ds(bases[h] + o, 16)
        shift = k_ref[rows, :]
        target = t_ref[rows, :] - base
        if tl_ref is not None:
            found = tl_ref[rows, :]
        for j in range(width // LANE):
            o = c * width + LANE * j
            x = get(r, o)
            hit = target == o
            p = jnp.exp2(x - shift)
            if tl_ref is not None:
                found = jnp.where(hit, x, found)
            dl_ref[16 * r:16 * r + 16, o:o + LANE] = jnp.where(hit, p - scale, p).astype(BF16)
        if tl_ref is not None:
            tl_ref[rows, :] = found


def pair_columns(a, b, c, d):
    return jnp.concatenate([jnp.concatenate([a[ALL], b[ALL]], axis=1), jnp.concatenate([c[ALL], d[ALL]], axis=1)], axis=0)


def own_kernel(sc, l_ref, e_ref, za0, za1, zb0, zb1, k_ref, t_ref, inv_ref, dz_ref, gv_ref, da_ref, db_ref, tl_ref, dl_ref, kw_ref, tw_ref, part_ref, acc_ref, sem):
    v, t = pl.program_id(0), pl.program_id(1)
    bases = spots(sc, 0)
    skip = sc[4, 3]

    expand(t, v, skip, bases, k_ref, t_ref, kw_ref, tw_ref)
    seq = acc_ref.shape[2]
    slots = [lax.bitwise_xor(lax.div(base, seq), sc[4, 0]) for base in bases]
    places = [pl.ds(pl.multiple_of(lax.rem(base, seq), LANE), LANE) for base in bases]

    @pl.when((v == 0) & (t >= skip))
    def _():
        for slot, place in zip(slots, places):
            acc_ref[slot, :, place] = jnp.zeros((acc_ref.shape[1], LANE), F32)

    @pl.when((v == 0) & (t == 0))
    def _():
        tl_ref[ALL] = jnp.zeros_like(tl_ref)

    @pl.when(t == skip)
    def _():
        da_ref[ALL] = jnp.zeros_like(da_ref)
        db_ref[ALL] = jnp.zeros_like(db_ref)

    @pl.when(t >= skip)
    def _():
        zc = pair_columns(za0, za1, zb0, zb1)
        half = za0.shape[0]
        scale = jnp.concatenate([inv_ref[ALL], inv_ref[ALL]], axis=0)
        n = VB // SC
        get = lambda r, o: l_ref[0, 0, 16 * r:16 * r + 16, o:o + LANE]
        for c in range(n + 1):
            if c < n:
                dlogits_stage(get, dl_ref, kw_ref, scale, tw_ref, tl_ref, bases, v * VB, c, SC)
            if c > 0:
                q = slice((c - 1) * SC, c * SC)
                dl = dl_ref[:, q]
                dz = lax.dot_general(e_ref[:, q], dl, (((1,), (1,)), ((), ())), preferred_element_type=F32)
                part_ref[ALL] = dz if c == 1 else part_ref[ALL] + dz
                de = jnp.dot(zc, dl, preferred_element_type=F32)
                da_ref[:, q] += de[:half]
                db_ref[:, q] += de[half:]
        for h, (slot, place) in enumerate(zip(slots, places)):
            acc_ref[slot, :, place] += part_ref[:, LANE * h:LANE * h + LANE]

    @pl.when((v == pl.num_programs(0) - 1) & (t == pl.num_programs(1) - 1))
    def _():
        copies = [pltpu.make_async_copy(acc_ref.at[k], out, sem.at[k]) for k, out in enumerate((dz_ref, gv_ref))]
        for copy in copies:
            copy.start()
        for copy in copies:
            copy.wait()


def other_kernel(sc, z0, z1, e_ref, za0, za1, zb0, zb1, k_ref, t_ref, inv_ref, ia_ref, ib_ref, da_ref, db_ref, l_ref, dl_ref, kw_ref, tw_ref):
    v, t = pl.program_id(0), pl.program_id(1)
    bases = spots(sc, 2)
    skip = sc[4, 4]
    expand(t, v, skip, bases, k_ref, t_ref, kw_ref, tw_ref)

    @pl.when(t == skip)
    def _():
        da_ref[ALL] = ia_ref[ALL]
        db_ref[ALL] = ib_ref[ALL]

    @pl.when(t >= skip)
    def _():
        zc = pair_columns(za0, za1, zb0, zb1)
        half = za0.shape[0]
        z = jnp.concatenate([z0[ALL], z1[ALL]], axis=0)
        scale = jnp.concatenate([inv_ref[ALL], inv_ref[ALL]], axis=0)
        n = VB // SF
        get = lambda r, o: l_ref[16 * r:16 * r + 16, o:o + LANE] * LOG2E
        for c in range(n + 2):
            if c < n:
                q = slice(c * SF, (c + 1) * SF)
                l_ref[:, q] = jnp.dot(z, e_ref[:, q], preferred_element_type=F32)
            if 0 < c <= n:
                dlogits_stage(get, dl_ref, kw_ref, scale, tw_ref, None, bases, v * VB, c - 1, SF)
            if c > 1:
                q = slice((c - 2) * SF, (c - 1) * SF)
                de = jnp.dot(zc, dl_ref[:, q], preferred_element_type=F32)
                da_ref[:, q] += de[:half]
                db_ref[:, q] += de[half:]


def swap_kernel(own_ref, give_ref, a_ref, b_ref, zt_ref, z_ref, dz_ref, got_ref, s_sem, r_sem):
    dp, tp = lax.axis_index("dp"), lax.axis_index("tp")
    i, n = pl.program_id(0), pl.num_programs(0)
    peer = (tp, xor(dp, 1))
    copy = link(give_ref, got_ref, (s_sem, r_sem), 0, peer)

    @pl.when(i == 0)
    def _():
        greet([peer])
        copy.start()

    z = jnp.where(i < 2, a_ref[ALL], b_ref[ALL]).astype(BF16)
    zt_ref[ALL] = z
    z_ref[ALL] = z.T

    @pl.when(i == n - 1)
    def _():
        copy.wait()
        dz_ref[ALL] = own_ref[ALL] + got_ref[ALL]


def xor(i, k):
    return (i + 1 - 2 * lax.rem(i, 2), lax.rem(i + 2, 4), 3 - i)[k - 1]


def expand(t, v, skip, bases, k_ref, t_ref, kw_ref, tw_ref):
    @pl.when((v == 0) & (t >= skip))
    def _():
        lane = lax.broadcasted_iota(jnp.int32, (1, LANE), 1)
        for base in bases:
            r = pl.ds(lax.div(base, LANE), 1)
            kw_ref[pl.ds(base, LANE), :] = columns(k_ref[r, :])
            tw_ref[pl.ds(base, LANE), :] = columns(t_ref[r, :]) - lane


def columns(row):
    return jnp.broadcast_to(row, (LANE, LANE)).T


def sort_lists(i_ref, ge_ref, outs, ids_ref, key_ref, perm_ref, sorted_ref):
    seq = i_ref.shape[1]
    nb = seq // LANE
    lane = lax.broadcasted_iota(jnp.int32, (1, LANE), 1)
    rows = [i_ref[:, LANE * j:LANE * j + LANE] * seq + lane + LANE * j for j in range(nb)]
    for j in range(nb):
        key_ref[LANE * j:LANE * j + LANE, :] = columns(rows[j])
    keys = key_ref[ALL]
    before = jnp.zeros((seq, LANE), F32)
    for j in range(nb):
        before = before + jnp.where(rows[j] < keys, 1.0, 0.0)
    rank = jnp.broadcast_to(over_lanes(before), (seq, LANE)).astype(jnp.int32)
    ids_ref[ALL] = jnp.zeros_like(ids_ref)
    for j in range(nb):
        hit = rank == lane + LANE * j
        perm_ref[:, LANE * j:LANE * j + LANE] = jnp.where(hit, 1.0, 0.0).astype(BF16)
        place = over_rows(jnp.where(hit, keys, 0))
        ids_ref[0:1, LANE * j:LANE * j + LANE] = lax.shift_right_logical(place, seq.bit_length() - 1)
    sorted_ref[ALL] = jnp.dot(ge_ref[ALL], perm_ref[ALL], preferred_element_type=F32)
    dp = lax.axis_index("dp")
    cols = outs[0].shape[0]
    for k, o in enumerate(outs):
        who = dp if k == 0 else xor(dp, k)
        o[ALL] = sorted_ref[pl.ds(pl.multiple_of(who * cols, 8), cols), :]


def greet(peers):
    barrier = pltpu.get_barrier_semaphore()
    for peer in peers:
        pl.semaphore_signal(barrier, inc=1, device_id=peer, device_id_type=pl.DeviceIdType.MESH)
    pl.semaphore_wait(barrier, len(peers))


def send(src, dst, sems, k, peer):
    copy = link(src, dst, sems, k, peer)
    copy.start()
    return copy


def link(src, dst, sems, k, peer):
    return pltpu.make_async_remote_copy(
        src_ref=src, dst_ref=dst, send_sem=sems[0].at[k], recv_sem=sems[1].at[k],
        device_id=peer, device_id_type=pl.DeviceIdType.MESH)


def prep_kernel(vocab_local, h_ref, g_ref, t_ref, m_ref, i_ref, ge_ref, z32_ref, zt_ref, z_ref, all_ref, table_ref, inv_ref, o1, o2, o3, o4,
                meta_ref, ids_ref, key_ref, perm_ref, sorted_ref, got_ref, box_ref, id_box_ref, s_sem, r_sem):
    dp, tp = lax.axis_index("dp"), lax.axis_index("tp")
    core = lax.rem(dp, 2)
    chip = lax.div(dp, 2)
    d, seq = h_ref.shape
    at = lambda i: (tp, i)
    peers = [at(xor(dp, k)) for k in (1, 2, 3)]
    meta_ref[ALL] = jnp.zeros_like(meta_ref)
    meta_ref[0:1, :] = t_ref[ALL]
    meta_ref[1:2, :] = m_ref[ALL]
    greet(peers)
    sems = (s_sem, r_sem)
    copies = [send(meta_ref, box_ref.at[k], sems, k, peers[k]) for k in range(3)]
    x = h_ref[ALL].astype(F32)
    inv = lax.rsqrt(mean_rows(x * x) + RMS_EPS)
    gain = jnp.concatenate([jnp.broadcast_to(g_ref[ALL].astype(F32)[None], (LANE, d)).T] * (seq // LANE), axis=1)
    z = (x * inv * gain).astype(BF16)
    z32_ref[ALL] = z.astype(F32)
    z_ref[pl.ds(pl.multiple_of(core * seq, seq), seq), :] = z.T
    copies.append(send(z32_ref, got_ref, sems, 3, peers[0]))
    zt_ref[:, pl.ds(pl.multiple_of(core * seq, seq), seq)] = z
    sort_lists(i_ref, ge_ref, (o1, o2, o3, o4), ids_ref, key_ref, perm_ref, sorted_ref)
    id_copies = [send(ids_ref, id_box_ref.at[k], sems, k + 4, peers[k]) for k in range(3)]
    for copy in copies[:3]:
        copy.wait()
    all_ref[dp] = meta_ref[ALL]
    for k in range(3):
        all_ref[xor(dp, k + 1)] = box_ref[k]

    tiles = []
    total = jnp.zeros((1, 1), F32)
    for q in range(4):
        length = over_lanes(all_ref[q, 1:2, :].astype(F32))
        total = total + length
        tiles.append(jnp.floor((length + (LANE - 1)) * (1.0 / LANE)).astype(jnp.int32))
    inv_ref[ALL] = jnp.broadcast_to(1.0 / total, inv_ref.shape)
    nt = 2 * seq // TB
    lane = lax.broadcasted_iota(jnp.int32, (1, LANE), 1)
    swap = chip == 1
    pairs = [(tiles[0], tiles[1]), (tiles[2], tiles[3])]
    out = []
    skips = []
    for c in range(2):
        na = jnp.where(swap, pairs[1 - c][0], pairs[c][0])
        nb = jnp.where(swap, pairs[1 - c][1], pairs[c][1])
        skip = nt - lax.shift_right_logical(na + nb + 1, 1)
        full = seq // LANE
        spare = jnp.minimum(jnp.where(na < full, na, full + nb), 2 * full - 1)
        for h in range(TB // LANE):
            p = 2 * jnp.maximum(lane - skip, 0) + h
            out.append(jnp.where(p < na, p, jnp.where(p < na + nb, full + p - na, spare)))
        skips.append(skip)
    row = jnp.where(lane == 0, core, jnp.where(lane == 1, dp, jnp.where(lane == 2, xor(dp, 1), jnp.where(lane == 3, skips[0], jnp.where(lane == 4, skips[1], tp * vocab_local)))))
    table_ref[ALL] = jnp.zeros_like(table_ref)
    for k, line in enumerate(out + [row]):
        table_ref[k:k + 1, :] = line

    copies[3].wait()
    other = xor(dp, 1) - 2 * chip
    got = got_ref[ALL].astype(BF16)
    z_ref[pl.ds(pl.multiple_of(other * seq, seq), seq), :] = got.T
    zt_ref[:, pl.ds(pl.multiple_of(other * seq, seq), seq)] = got
    for copy in id_copies:
        copy.wait()
    all_ref[dp, 2:3, :] = ids_ref[0:1, :]
    for k in range(3):
        all_ref[xor(dp, k + 1), 2:3, :] = id_box_ref[k, 0:1, :]


def stats_kernel(vocab_local, m_ref, s_ref, all_ref, k_ref, t_ref, f_ref, lse_ref, look_ref, mine_ref, box_ref, s_sem, r_sem):
    dp, tp = lax.axis_index("dp"), lax.axis_index("tp")
    core = lax.rem(dp, 2)
    chip = lax.div(dp, 2)
    seq = all_ref.shape[2]
    nb = m_ref.shape[0] // LANE
    peers = [(tp, xor(dp, 1)), (1 - tp, dp), (1 - tp, xor(dp, 1))]
    greet(peers)
    for j in range(nb):
        m = m_ref[LANE * j:LANE * j + LANE, :].T
        s = s_ref[LANE * j:LANE * j + LANE, :].T
        top = jnp.max(m, axis=0, keepdims=True)
        mine_ref[j:j + 1, :] = top
        mine_ref[nb + j:nb + j + 1, :] = over_rows(s * jnp.exp2(m - top))
    copies = [send(mine_ref, box_ref.at[k], (s_sem, r_sem), k, peers[k]) for k in range(3)]

    lane = lax.broadcasted_iota(jnp.int32, (1, LANE), 1)
    edge = lane * LB + tp * vocab_local
    look_ref[ALL] = jnp.zeros_like(look_ref)
    steps = jnp.zeros((1, LANE), F32)
    for q in range(4):
        lo = jnp.zeros((1, LANE), F32)
        hi = jnp.zeros((1, LANE), F32)
        who = dp if q == 0 else xor(dp, q)
        for j in range(seq // LANE):
            ids = columns(all_ref[who, 2:3, LANE * j:LANE * j + LANE])
            lo = lo + over_rows(jnp.where(ids < edge, 1.0, 0.0))
            hi = hi + over_rows(jnp.where(ids < edge + LB, 1.0, 0.0))
        a = jnp.floor(lo * (1.0 / ST)) * ST
        look_ref[q:q + 1, :] = a.astype(jnp.int32)
        steps = jnp.maximum(steps, jnp.floor((hi - a + (CH - 1)) * (1.0 / CH)))
    look_ref[4:5, :] = steps.astype(jnp.int32)

    total = sum(over_lanes(all_ref[q, 1:2, :].astype(F32)) for q in range(4))
    shift = jnp.log(total) * LOG2E
    base = tp * vocab_local + core * (vocab_local // 2)
    half = nb // 2
    for c, out in ((chip, t_ref), (1 - chip, f_ref)):
        for j in range(nb):
            q, o = c * 2 + j // half, LANE * (j % half)
            on = all_ref[q, 1:2, o:o + LANE] > 0
            out[j:j + 1, :] = jnp.where(on, all_ref[q, 0:1, o:o + LANE] - base, -MIB)
    for copy in copies:
        copy.wait()
    parts = [mine_ref] + [box_ref.at[k] for k in range(3)]
    ms = [p[0:nb, :] for p in parts]
    top = functools.reduce(jnp.maximum, ms)
    w = [p[nb:2 * nb, :] * jnp.exp2(m - top) for p, m in zip(parts, ms)]
    lse = top + jnp.log((w[0] + w[1]) + (w[2] + w[3])) * LOG2E
    live = t_ref[ALL] > 1 - MIB
    k_ref[ALL] = jnp.where(live, lse + shift, jnp.inf)
    lse_ref[ALL] = jnp.broadcast_to(over_rows(jnp.where(live, lse, 0.0)), lse_ref.shape)


def final_kernel(a_ref, b_ref, h_ref, g_ref, on_ref, tl_ref, lse_ref, inv_ref, dh_ref, dg_ref, loss_ref, mine_ref, box_ref, s_sem, r_sem):
    dp, tp = lax.axis_index("dp"), lax.axis_index("tp")
    dps = [dp, xor(dp, 1), xor(dp, 2), xor(dp, 3)]
    peers = [(t, i) for t in (tp, 1 - tp) for i in dps][1:]
    greet(peers)
    d, seq = h_ref.shape
    x = h_ref[ALL].astype(F32)
    inv = lax.rsqrt(mean_rows(x * x) + RMS_EPS)
    u = x * inv
    dz = jnp.where(on_ref[ALL] > 0, a_ref[ALL] + b_ref[ALL], 0.0)
    prod = dz * u
    part = sum(prod[:, LANE * j:LANE * j + LANE] for j in range(seq // LANE))
    mine_ref[ALL] = jnp.zeros_like(mine_ref)
    mine_ref[0:1, 0:d] = over_rows(part.T)
    mine_ref[1:2, 0:LANE] = over_rows(tl_ref[ALL])
    mine_ref[2:3, 0:LANE] = lse_ref[0:1, :]
    box_ref[0] = mine_ref[ALL]
    copies = [send(mine_ref, box_ref.at[k + 1], (s_sem, r_sem), k, peers[k]) for k in range(7)]
    gain = jnp.concatenate([jnp.broadcast_to(g_ref[ALL].astype(F32)[None], (LANE, d)).T] * (seq // LANE), axis=1)
    w = dz * gain
    dh_ref[ALL] = (inv * (w - u * mean_rows(w * u))).astype(BF16)
    for copy in copies:
        copy.wait()
    same = [jnp.zeros((1, d), F32)] * 4
    found = jnp.zeros((1, LANE), F32)
    for q in range(4):
        row = jnp.zeros((1, d), F32)
        hit = jnp.zeros((1, LANE), F32)
        low = jnp.zeros((1, LANE), F32)
        for k in range(4):
            row = jnp.where(dps[k] == q, box_ref[k, 0:1, 0:d], row)
            hit = jnp.where(dps[k] == q, box_ref[k, 1:2, 0:LANE], hit)
            low = jnp.where(dps[k] == q, box_ref[k + 4, 1:2, 0:LANE], low)
        same[q] = row
        found = found + (hit + low)
    dg_ref[ALL] = (same[0] + same[1] + same[2] + same[3])[0]
    loss = over_lanes(box_ref[0, 2:3, 0:LANE] + box_ref[2, 2:3, 0:LANE] - found) * LN2
    loss_ref[ALL] = jnp.broadcast_to(loss, loss_ref.shape) * inv_ref[0:1, :]


def lookup_kernel(top, sc, look, from_ref, g1, g2, g3, g4, all_ref, *rest):
    out_ref, id_ref, row_ref = rest[-3:]
    b = pl.program_id(0)
    seq = all_ref.shape[2]
    lists = (g1, g2, g3, g4)

    @pl.when(b == 0)
    def _():
        for q, g in enumerate(lists):
            who = sc[4, 1] if q == 0 else xor(sc[4, 1], q)
            for j in range(seq // LANE):
                id_ref[q, LANE * j:LANE * j + LANE, :] = columns(all_ref[who, 2:3, LANE * j:LANE * j + LANE]) - sc[4, 5]
            row_ref[q, 0:seq, :] = g[ALL].astype(BF16).T
            id_ref[q, seq:, :] = jnp.full((CH, LANE), -MIB, jnp.int32)
            row_ref[q, seq:, :] = jnp.zeros((CH, row_ref.shape[2]), BF16)

    lane = lax.broadcasted_iota(jnp.int32, (CH, LB), 1)
    subs = from_ref.shape[1] // LB

    def part(at, k):
        hots, rows = [], []
        for q in range(len(lists)):
            c = pl.ds(pl.multiple_of(jnp.minimum(look[q, at] + k * CH, seq), ST), CH)
            ids = jnp.concatenate([id_ref[q, c, :] - at * LB] * (LB // LANE), axis=1)
            hots.append(jnp.where(ids == lane, 1.0, 0.0).astype(BF16))
            rows.append(row_ref[q, c, :])
        return lax.dot_general(
            jnp.concatenate(rows, axis=0), jnp.concatenate(hots, axis=0), (((0,), (0,)), ((), ())), preferred_element_type=F32)

    for u in range(subs):
        q = slice(u * LB, (u + 1) * LB)
        out_ref[:, q] = from_ref[:, q] + part(top(sc, b) * subs + u, 0)
    for u in range(subs):
        at = top(sc, b) * subs + u
        q = slice(u * LB, (u + 1) * LB)

        def step(k, _, at=at, q=q):
            out_ref[:, q] += part(at, k)
            return 0

        lax.fori_loop(1, look[4, at], step, 0)


def solution(mesh):
    n_dp = mesh.shape["dp"]
    swap = {k: [(i, i ^ k) for i in range(n_dp)] for k in (1, 2, 3)}

    def blocks(*arrays):
        return [pl.BlockSpec(a.shape, lambda i, n=len(a.shape): (0,) * n) for a in arrays]

    shape = jax.ShapeDtypeStruct

    def single(kernel, args, outs, scratch, ident=None):
        talk = {} if ident is None else dict(collective_id=ident, has_side_effects=True)
        return pl.pallas_call(
            kernel, grid=(1,), in_specs=blocks(*args), out_specs=blocks(*outs), out_shape=outs, scratch_shapes=scratch,
            compiler_params=pltpu.CompilerParams(dimension_semantics=("arbitrary",), vmem_limit_bytes=GRANT, **talk),
            cost_estimate=cost(SMALL))(*args)

    dma = pltpu.SemaphoreType.DMA

    def local_step(hidden, norm_w, embed, targets, loss_mask, token_ids, grad_embed):
        _, seq, d = hidden.shape
        vocab_local = embed.shape[0]
        half = vocab_local // 2
        nv = half // VB
        cols = d // n_dp
        nt = 2 * seq // TB
        et = embed.T
        ht = hidden[0].T

        zt32, zt_chip, z_chip, metas, table, inv_n, *give = single(
            functools.partial(prep_kernel, vocab_local),
            (ht, norm_w, targets, loss_mask, token_ids, grad_embed[0].T),
            [shape((d, seq), F32), shape((d, 2 * seq), BF16), shape((2 * seq, d), BF16),
             shape((n_dp, 8, seq), jnp.int32), shape((8, LANE), jnp.int32), shape((8, LANE), F32)] + [shape((cols, seq), F32)] * 4,
            [pltpu.VMEM((8, seq), jnp.int32), pltpu.VMEM((8, seq), jnp.int32),
             pltpu.VMEM((seq, LANE), jnp.int32), pltpu.VMEM((seq, seq), BF16), pltpu.VMEM((d, seq), F32),
             pltpu.VMEM((d, seq), F32), pltpu.VMEM((3, 8, seq), jnp.int32), pltpu.VMEM((3, 8, seq), jnp.int32),
             dma((7,)), dma((7,))], 0)

        far = lax.ppermute(zt32, "dp", swap[2])
        far_near = lax.ppermute(far, "dp", swap[1])

        def swap_call(own, give, a, b):
            w = seq // 2
            return pl.pallas_call(
                swap_kernel, grid=(4,),
                in_specs=[pl.BlockSpec((d, seq), lambda i: (0, 0)), pl.BlockSpec(memory_space=pl.ANY),
                          pl.BlockSpec((d, w), lambda i: (0, jnp.minimum(i, 1))), pl.BlockSpec((d, w), lambda i: (0, jnp.maximum(i - 2, 0)))],
                out_specs=[pl.BlockSpec((d, w), lambda i: (0, i)), pl.BlockSpec((w, d), lambda i: (i, 0)), pl.BlockSpec((d, seq), lambda i: (0, 0))],
                out_shape=[shape((d, 2 * seq), BF16), shape((2 * seq, d), BF16), shape((d, seq), F32)],
                scratch_shapes=[pltpu.VMEM((d, seq), F32), dma((1,)), dma((1,))],
                compiler_params=pltpu.CompilerParams(
                    dimension_semantics=("arbitrary",), vmem_limit_bytes=GRANT, collective_id=3, has_side_effects=True),
                name="swap", cost_estimate=cost(SMALL))(own, give, a, b)

        def specs(r):
            at = lambda x, t, h: lax.bitwise_xor(x[r + h, t], x[4, 0] * (seq // LANE)) if r else x[h, t]
            full = lambda v, t, x: (0, 0)
            halves = range(TB // LANE)
            return dict(
                e=[pl.BlockSpec((d, VB), lambda v, t, x: (0, x[4, 0] * nv + v))],
                z=[pl.BlockSpec((LANE, d), lambda v, t, x, h=h: (at(x, t, h), 0)) for h in halves],
                l=[pl.BlockSpec((1, 1, TB, VB), lambda v, t, x: (jnp.maximum(t, x[4, 3]), v, 0, 0))],
                vec=[pl.BlockSpec((2 * seq, LANE), full)],
                row=[pl.BlockSpec((2 * seq // LANE, LANE), full)],
                any=[pl.BlockSpec(memory_space=pl.ANY)],
                inv=[pl.BlockSpec((8, LANE), full)],
                zc=[pl.BlockSpec((cols, LANE), lambda v, t, x, h=h, k=k: (x[4, k], at(x, t, h))) for k in (1, 2) for h in halves],
                de=[pl.BlockSpec((cols, VB), lambda v, t, x: (0, v))])

        pick = lambda sp, *names: [b for k in names for b in sp[k]]
        own, other = specs(0), specs(2)
        vec = shape((2 * seq, LANE), F32)
        wide = [pltpu.VMEM((2 * seq, LANE), F32), pltpu.VMEM((2 * seq, LANE), jnp.int32)]
        de_shape = shape((cols, half), F32)
        flops = 2 * 2 * seq * half * d

        l_own, m_own, s_own = pl.pallas_call(
            logits_kernel,
            grid_spec=pltpu.PrefetchScalarGridSpec(
                num_scalar_prefetch=1, grid=(nv, nt), in_specs=pick(own, "z", "e"), out_specs=pick(own, "l", "vec", "vec")),
            out_shape=[shape((nt, nv, TB, VB), F32), vec, vec],
            compiler_params=params(), name="logits",
            cost_estimate=cost(flops),
        )(table, z_chip, z_chip, et)

        rows = 2 * seq // LANE
        k_own, t_own, t_far, lse_sum, look = single(
            functools.partial(stats_kernel, vocab_local), (m_own, s_own, metas),
            [shape((rows, LANE), F32), shape((rows, LANE), jnp.int32), shape((rows, LANE), jnp.int32),
             shape((8, LANE), F32), shape((8, LANE), jnp.int32)],
            [pltpu.VMEM((2 * rows, LANE), F32), pltpu.VMEM((3, 2 * rows, LANE), F32), dma((3,)), dma((3,))], 1)
        k_far = lax.ppermute(k_own, "dp", swap[2])

        lists = [give[0]]
        for k in (1, 2, 3):
            lists.append(lax.ppermute(give[k], "dp", swap[k]))

        dz_own, dz_give, da, db, tl = pl.pallas_call(
            own_kernel,
            grid_spec=pltpu.PrefetchScalarGridSpec(
                num_scalar_prefetch=1, grid=(nv, nt),
                in_specs=pick(own, "l", "e", "zc", "row", "row", "inv"), out_specs=pick(own, "any", "any", "de", "de", "vec"),
                scratch_shapes=[pltpu.VMEM((TB, VB), BF16), *wide, pltpu.VMEM((d, TB), F32), pltpu.VMEM((2, d, seq), F32), dma((2,))]),
            out_shape=[shape((d, seq), F32), shape((d, seq), F32), de_shape, de_shape, vec],
            compiler_params=params(), name="own",
            cost_estimate=cost(flops + flops // 2),
        )(table, l_own, et, *[zt_chip] * 4, k_own, t_own, inv_n)

        zt_far, z_far, dz_half = swap_call(dz_own, dz_give, far, far_near)
        dz_tp = lax.ppermute(dz_half, "tp", [(0, 1), (1, 0)])

        da, db = pl.pallas_call(
            other_kernel,
            grid_spec=pltpu.PrefetchScalarGridSpec(
                num_scalar_prefetch=1, grid=(nv, nt),
                in_specs=pick(other, "z", "e", "zc", "row", "row", "inv", "de", "de"), out_specs=pick(other, "de", "de"),
                scratch_shapes=[pltpu.VMEM((TB, VB), F32), pltpu.VMEM((TB, VB), BF16), *wide]),
            out_shape=[de_shape, de_shape],
            compiler_params=params(), name="other",
            cost_estimate=cost(flops + flops // 2),
        )(table, z_far, z_far, et, *[zt_far] * 4, k_far, t_far, inv_n, da, db)
        got = lax.ppermute(db, "dp", swap[1])

        nb = half // LW

        def lookup(top, source, *prior):
            zero = lambda b, x, k: (0, 0)
            return pl.pallas_call(
                functools.partial(lookup_kernel, top),
                grid_spec=pltpu.PrefetchScalarGridSpec(
                    num_scalar_prefetch=2, grid=(nb,),
                    in_specs=[pl.BlockSpec((cols, LW), lambda b, x, k: (0, b))] + [pl.BlockSpec((cols, seq), zero)] * 4
                    + [pl.BlockSpec((n_dp, 8, seq), lambda b, x, k: (0, 0, 0))] + [pl.BlockSpec(memory_space=pl.ANY)] * len(prior),
                    out_specs=pl.BlockSpec((cols, LW), lambda b, x, k: (0, top(x, b))),
                    scratch_shapes=[pltpu.VMEM((4, seq + CH, LANE), jnp.int32), pltpu.VMEM((4, seq + CH, cols), BF16)]),
                out_shape=shape((cols, vocab_local), F32),
                input_output_aliases={8: 0} if prior else {},
                compiler_params=params(1), name="lookup",
                cost_estimate=cost(flops // 8),
            )(table, look, source, *lists, metas, *prior)

        de_t = lookup(lambda x, b: x[4, 0] * nb + b, da)

        dht, dg, loss = single(
            final_kernel, (dz_half, dz_tp, ht, norm_w, loss_mask, tl, lse_sum, inv_n),
            [shape((d, seq), BF16), shape((d,), F32), shape((1, LANE), F32)],
            [pltpu.VMEM((8, 640), F32), pltpu.VMEM((8, 8, 640), F32), dma((7,)), dma((7,))], 2)

        de_t = lookup(lambda x, b: (1 - x[4, 0]) * nb + b, got, de_t)
        return loss[0, 0], dht.T[None], dg, de_t.T

    return jax.shard_map(
        local_step, mesh=mesh,
        in_specs=(P("dp"), P(), P("tp"), P("dp"), P("dp"), P("dp"), P("dp")),
        out_specs=(P(), P("dp"), P(), P("tp", "dp")), check_vma=False)
```
